8 devices in a mesh: dp: 1 (over z), cp: 8 (over y, x, core).
Axes of the slice: x: 2, y: 2, z: 1, core: 2. Of those that a mesh axis runs over, the one named last changes fastest.
Arguments:
- hidden: bfloat16 [3, 1024, 2560], P('dp', 'cp')
- positions: int32 [3, 1024], P('dp', 'cp')
- wq_local: bfloat16 [2560, 2048], replicated
- wk_local: bfloat16 [2560, 1024], replicated
- wv_local: bfloat16 [2560, 1024], replicated
- wo_local: bfloat16 [2048, 2560], replicated
- wgate_local: bfloat16 [2560, 10240], replicated
- wup_local: bfloat16 [2560, 10240], replicated
- wdown_local: bfloat16 [10240, 2560], replicated
- preatt_local: float32 [2560], replicated
- postatt_local: float32 [2560], replicated
- preffw_local: float32 [2560], replicated
- postffw_local: float32 [2560], replicated
- wq_global: bfloat16 [2560, 2048], replicated
- wk_global: bfloat16 [2560, 1024], replicated
- wv_global: bfloat16 [2560, 1024], replicated
- wo_global: bfloat16 [2048, 2560], replicated
- wgate_global: bfloat16 [2560, 10240], replicated
- wup_global: bfloat16 [2560, 10240], replicated
- wdown_global: bfloat16 [10240, 2560], replicated
- preatt_global: float32 [2560], replicated
- postatt_global: float32 [2560], replicated
- preffw_global: float32 [2560], replicated
- postffw_global: float32 [2560], replicated
Outputs:
- output: bfloat16 [3, 1024, 2560], P('dp', 'cp')
All inputs are finite; a program needn't handle non-finite values.
Results may differ from the reference program's by a relative error of at most 0.02.
Values are sent between devices in bfloat16 or wider.
A program may use at most 1.5 GiB of HBM per device.

```python
import jax
import jax.numpy as jnp
from jax import lax

BATCH_ROWS = 3
SEQ_LEN = 1024
BLOCK_LEN = 128
MODEL_DIM = 2560
NUM_HEADS = 8
KV_HEADS = 4
HEAD_DIM = 256
FFN_DIM = 10240
WINDOW = 512
NUM_BLOCKS = SEQ_LEN // BLOCK_LEN
GROUP_SIZE = NUM_HEADS // KV_HEADS
EPSILON = 1e-6
THETA = 10000.0
SOFT_CAP = 50.0
LAYER_TAGS = ("local", "global")
WEIGHT_NAMES = ("wq", "wk", "wv", "wo", "wgate", "wup", "wdown")
SCALE_NAMES = ("preatt", "postatt", "preffw", "postffw")


def layer_weights(rng_key, layer_tag):
    key_list = jax.random.split(rng_key, 11)
    q_width = NUM_HEADS * HEAD_DIM
    kv_width = KV_HEADS * HEAD_DIM
    shapes = ((MODEL_DIM, q_width), (MODEL_DIM, kv_width), (MODEL_DIM, kv_width), (q_width, MODEL_DIM), (MODEL_DIM, FFN_DIM), (MODEL_DIM, FFN_DIM), (FFN_DIM, MODEL_DIM))
    weights = {}
    for slot_idx in range(7):
        fan_in, fan_out = shapes[slot_idx]
        drawn = jax.random.normal(key_list[slot_idx], (fan_in, fan_out), jnp.float32) * fan_in ** -0.5
        weights[WEIGHT_NAMES[slot_idx] + "_" + layer_tag] = drawn.astype(jnp.bfloat16)
    for slot_idx in range(4):
        weights[SCALE_NAMES[slot_idx] + "_" + layer_tag] = 0.4 * jax.random.normal(key_list[7 + slot_idx], (MODEL_DIM,), jnp.float32)
    return weights


def setup_inputs(seed: int = 0, part: int = 0) -> dict:
    part_key = jax.random.fold_in(jax.random.key(seed), part)
    key_hidden, key_steps = jax.random.split(part_key)
    hidden = jax.random.normal(key_hidden, (BATCH_ROWS, SEQ_LEN, MODEL_DIM), jnp.float32).astype(jnp.bfloat16)
    step_sizes = jax.random.randint(key_steps, (BATCH_ROWS, SEQ_LEN), 1, 3, jnp.int32)
    positions = (jnp.cumsum(step_sizes, axis=1) - step_sizes[:, :1]).astype(jnp.int32)
    inputs = {"hidden": hidden, "positions": positions}
    weight_key = jax.random.key(seed + 1)
    for layer_idx in range(2):
        inputs.update(layer_weights(jax.random.fold_in(weight_key, layer_idx), LAYER_TAGS[layer_idx]))
    return inputs


def rms_norm(inputs, norm_scale):
    widened = inputs.astype(jnp.float32)
    mean_sq = jnp.mean(widened * widened, axis=-1, keepdims=True)
    return (widened * lax.rsqrt(mean_sq + EPSILON) * (1.0 + norm_scale)).astype(jnp.bfloat16)


def mat_mul(inputs, weight):
    flat_in = inputs.reshape(-1, inputs.shape[-1])
    product = jnp.dot(flat_in, weight, preferred_element_type=jnp.float32)
    return product.reshape(inputs.shape[:-1] + (weight.shape[1],)).astype(jnp.bfloat16)


def apply_rope(heads_in, positions):
    half_dim = HEAD_DIM // 2
    inv_freq = THETA ** (-(jnp.arange(half_dim, dtype=jnp.float32) * 2.0 / HEAD_DIM))
    angles = positions.astype(jnp.float32)[:, :, None, None] * inv_freq
    cos_t = jnp.cos(angles)
    sin_t = jnp.sin(angles)
    widened = heads_in.astype(jnp.float32)
    first_half = widened[..., :half_dim]
    second_half = widened[..., half_dim:]
    return jnp.concatenate([first_half * cos_t - second_half * sin_t, second_half * cos_t + first_half * sin_t], axis=-1)


def decoder_layer(hidden, positions, weights, window_len):
    w_q, w_k, w_v, w_o, w_gate, w_up, w_down, pre_att, post_att, pre_ffw, post_ffw = weights
    normed = rms_norm(hidden, pre_att)
    query_rot = apply_rope(mat_mul(normed, w_q).reshape(BATCH_ROWS, SEQ_LEN, NUM_HEADS, HEAD_DIM), positions)
    query_rot = (query_rot * HEAD_DIM ** -0.5).astype(jnp.bfloat16)
    key_rot = apply_rope(mat_mul(normed, w_k).reshape(BATCH_ROWS, SEQ_LEN, KV_HEADS, HEAD_DIM), positions).astype(jnp.bfloat16)
    value_t = mat_mul(normed, w_v).reshape(BATCH_ROWS, SEQ_LEN, KV_HEADS, HEAD_DIM)
    key_wide = key_rot.astype(jnp.float32)
    value_wide = value_t.astype(jnp.float32)
    q_blocks = query_rot.reshape(BATCH_ROWS, NUM_BLOCKS, BLOCK_LEN, KV_HEADS, GROUP_SIZE, HEAD_DIM).transpose(1, 0, 2, 3, 4, 5)
    pos_blocks = positions.reshape(BATCH_ROWS, NUM_BLOCKS, BLOCK_LEN).transpose(1, 0, 2)
    hid_blocks = hidden.reshape(BATCH_ROWS, NUM_BLOCKS, BLOCK_LEN, MODEL_DIM).transpose(1, 0, 2, 3)

    def one_block(block_in):
        q_block, q_pos, h_block = block_in
        scores = jnp.einsum("bqkgd,bskd->bkgqs", q_block.astype(jnp.float32), key_wide)
        capped = SOFT_CAP * jnp.tanh(scores / SOFT_CAP)
        offset = q_pos[:, None, None, :, None] - positions[:, None, None, None, :]
        visible = (offset >= 0) & (offset < window_len)
        prob_bf = jax.nn.softmax(jnp.where(visible, capped, -1e30), axis=-1).astype(jnp.bfloat16)
        mixed_heads = jnp.einsum("bkgqs,bskd->bqkgd", prob_bf.astype(jnp.float32), value_wide).astype(jnp.bfloat16)
        attn_out = mat_mul(mixed_heads.reshape(BATCH_ROWS, BLOCK_LEN, NUM_HEADS * HEAD_DIM), w_o)
        mid_state = (h_block.astype(jnp.float32) + rms_norm(attn_out, post_att).astype(jnp.float32)).astype(jnp.bfloat16)
        normed_mid = rms_norm(mid_state, pre_ffw)
        gate_val = mat_mul(normed_mid, w_gate)
        up_val = mat_mul(normed_mid, w_up)
        act_val = (jax.nn.gelu(gate_val.astype(jnp.float32), approximate=True) * up_val.astype(jnp.float32)).astype(jnp.bfloat16)
        down_val = mat_mul(act_val, w_down)
        return (mid_state.astype(jnp.float32) + rms_norm(down_val, post_ffw).astype(jnp.float32)).astype(jnp.bfloat16)

    out_blocks = lax.map(one_block, (q_blocks, pos_blocks, hid_blocks))
    return out_blocks.transpose(1, 0, 2, 3).reshape(BATCH_ROWS, SEQ_LEN, MODEL_DIM)


def reference(hidden, positions, wq_local, wk_local, wv_local, wo_local, wgate_local, wup_local, wdown_local, preatt_local, postatt_local, preffw_local, postffw_local, wq_global, wk_global, wv_global, wo_global, wgate_global, wup_global, wdown_global, preatt_global, postatt_global, preffw_global, postffw_global):
    local_set = (wq_local, wk_local, wv_local, wo_local, wgate_local, wup_local, wdown_local, preatt_local, postatt_local, preffw_local, postffw_local)
    global_set = (wq_global, wk_global, wv_global, wo_global, wgate_global, wup_global, wdown_global, preatt_global, postatt_global, preffw_global, postffw_global)
    mid_hidden = decoder_layer(hidden, positions, local_set, WINDOW)
    return decoder_layer(mid_hidden, positions, global_set, 2 * SEQ_LEN)
```

```python
import functools
import math

import jax
import jax.numpy as jnp
from jax import lax
from jax.experimental import pallas as pl
from jax.experimental.pallas import tpu as pltpu
from jax.sharding import PartitionSpec as P

HEAD_DIM = 256
WINDOW = 512
EPSILON = 1e-6
THETA = 10000.0
SOFT_CAP = 50.0
EXP2_CAP = SOFT_CAP * math.log2(math.e)

MESH = pl.DeviceIdType.MESH
F32 = jnp.float32
BF16 = jnp.bfloat16

ROWS = 3
TOK = 128
CTOK = 256
DIM = 2560
HQ = 1024
HKV = 512
FF = 10240
FFH = FF // 2
DH = DIM // 2
CHIPS = 4
STEPS = 2 * ROWS
DEPTH = 4
GU = FFH // 512


def dot(a, b):
    return jnp.dot(a, b, preferred_element_type=F32)


def rms(u, w):
    mean_sq = jnp.mean(u * u, axis=-1, keepdims=True)
    return (u * lax.rsqrt(mean_sq + EPSILON) * (1.0 + w)).astype(BF16)


def gated(g, u):
    g = g.astype(BF16).astype(F32)
    u = u.astype(BF16).astype(F32)
    return (jax.nn.gelu(g, approximate=True) * u).astype(BF16)


def kernel(x_hbm, tab_in, pos_in, norms,
           wq0, wk0, wv0, wo0, wg0, wu0, wd0, wq1, wk1, wv1, wo1, wg1, wu1, wd1,
           out_hbm,
           ring, kvbuf, xbuf, mbuf, hbuf, qbuf, obuf, abuf, dbuf, tab, posbuf, ebuf, gs, us,
           ring_sem, xl_sem, xs_sem, xr_sem, ts_sem, tr_sem, ps_sem, pr_sem, kvs_sem, kvr_sem,
           os_sem, or_sem, as_sem, ar_sem, hs_sem, hr_sem, dss_sem, dr_sem, out_sem):
    me = lax.axis_index("cp")
    chip = me // 2
    core = me % 2
    peer = me + 1 - 2 * core

    def at(dev):
        return {"cp": dev}

    def start_cols(w, rows, col, slot, row0):
        pltpu.make_async_copy(
            w.at[pl.ds(0, rows), pl.ds(pl.multiple_of(col, 256), 256)],
            ring.at[slot, pl.ds(row0, rows), :], ring_sem.at[slot]).start()

    def by_layer(first, f0, f1):
        @pl.when(first)
        def _():
            f0()

        @pl.when(jnp.logical_not(first))
        def _():
            f1()

    def start_gu(first, i, slot):
        def go(wg, wu):
            col = core * FFH + i * 512
            for t in range(2):
                start_cols(wg, DIM, col + 256 * t, slot, 2 * t * DIM)
                start_cols(wu, DIM, col + 256 * t, slot, (2 * t + 1) * DIM)
        by_layer(first, lambda: go(wg0, wu0), lambda: go(wg1, wu1))

    def start_down(first, n, slot):
        def go(wd):
            start_cols(wd, FF, core * DH + n * 256, slot, 0)
        by_layer(first, lambda: go(wd0), lambda: go(wd1))

    def start_wo(first, slot):
        def go(wo):
            for t in range(5):
                start_cols(wo, 2048, core * DH + t * 256, slot, t * 2048)
        by_layer(first, lambda: go(wo0), lambda: go(wo1))

    def start_kv(wk, wv, slot):
        for t in range(2):
            start_cols(wk, DIM, core * HKV + t * 256, slot, t * DIM)
            start_cols(wv, DIM, core * HKV + t * 256, slot, (2 + t) * DIM)

    def start_q(wq, slot):
        for t in range(4):
            start_cols(wq, DIM, core * HQ + t * 256, slot, t * DIM)

    def wait_w(slot):
        pltpu.make_async_copy(wd0.at[:, pl.ds(0, 256)], ring.at[slot], ring_sem.at[slot]).wait()

    def unit(slot, t, rows=DIM):
        return ring[slot, pl.ds(t * rows, rows), :]

    def x_local(r):
        return pltpu.make_async_copy(
            x_hbm.at[r], xbuf.at[r, pl.ds(pl.multiple_of(core * TOK, TOK), TOK), :], xl_sem.at[r])

    def x_remote(r):
        return pltpu.make_async_remote_copy(
            x_hbm.at[r], xbuf.at[r, pl.ds(pl.multiple_of(core * TOK, TOK), TOK), :],
            xs_sem.at[r], xr_sem.at[r], device_id=at(peer), device_id_type=MESH)

    def tab_local():
        return pltpu.make_async_copy(tab_in, tab.at[core], ts_sem.at[0])

    def tab_remote():
        return pltpu.make_async_remote_copy(
            tab_in, tab.at[core], ts_sem.at[1], tr_sem.at[0], device_id=at(peer), device_id_type=MESH)

    def pos_local():
        return pltpu.make_async_copy(pos_in, posbuf.at[me], ps_sem.at[0])

    def pos_remote(k):
        return pltpu.make_async_remote_copy(
            pos_in, posbuf.at[me], ps_sem.at[k], pr_sem.at[k],
            device_id=at(lax.rem(me + k, 8)), device_id_type=MESH)

    def kv_remote(l, r, d):
        return pltpu.make_async_remote_copy(
            kvbuf.at[l, r, chip], kvbuf.at[l, r, chip], kvs_sem.at[l, r, d], kvr_sem.at[l, r, d],
            device_id=at(lax.rem(me + 2 * d, 8)), device_id_type=MESH)

    def half(buf, width):
        return buf.at[:, pl.ds(pl.multiple_of(core * width, 256), width)]

    def o_remote():
        return pltpu.make_async_remote_copy(
            half(obuf, HQ), half(obuf, HQ), os_sem, or_sem, device_id=at(peer), device_id_type=MESH)

    def a_remote():
        return pltpu.make_async_remote_copy(
            half(abuf, DH), half(abuf, DH), as_sem, ar_sem, device_id=at(peer), device_id_type=MESH)

    def d_remote(par):
        return pltpu.make_async_remote_copy(
            half(dbuf.at[par], DH), half(dbuf.at[par], DH), dss_sem.at[par], dr_sem.at[par],
            device_id=at(peer), device_id_type=MESH)

    def h_remote(par, i):
        w = hbuf.at[par, :, pl.ds(pl.multiple_of(core * FFH + i * 512, 512), 512)]
        return pltpu.make_async_remote_copy(
            w, w, hs_sem.at[par], hr_sem.at[par], device_id=at(peer), device_id_type=MESH)

    def h_all(par):
        w = hbuf.at[par, :, pl.ds(pl.multiple_of(core * FFH, 512), FFH)]
        return pltpu.make_async_remote_copy(
            w, w, hs_sem.at[par], hr_sem.at[par], device_id=at(peer), device_id_type=MESH)

    def rope(y, r, t, dst):
        y = y.astype(BF16).astype(F32)
        for c in range(2):
            f = y[c * TOK:(c + 1) * TOK, :128]
            s = y[c * TOK:(c + 1) * TOK, 128:]
            cos = tab[c, r, 0]
            sin = tab[c, r, 1]
            dst(c, (f * cos - s * sin) * t, (s * cos + f * sin) * t)

    def kv_part(src, slot, l, r):
        for t in range(2):
            y = dot(src(), unit(slot, t))

            def put(c, a, b, t=t):
                rows = pl.ds(c * TOK, TOK)
                kvbuf[l, r, chip, rows, t * 256:t * 256 + 128] = a.astype(BF16)
                kvbuf[l, r, chip, rows, t * 256 + 128:t * 256 + 256] = b.astype(BF16)
            rope(y, r, 1.0, put)
            kvbuf[l, r, chip, :, HKV + t * 256:HKV + t * 256 + 256] = dot(src(), unit(slot, 2 + t)).astype(BF16)

    def q_part(src, slot, r):
        for t in range(4):
            y = dot(src(), unit(slot, t))

            def put(c, a, b, t=t):
                rows = pl.ds(c * TOK, TOK)
                qbuf[r, t, rows, 0:128] = a.astype(BF16)
                qbuf[r, t, rows, 128:256] = b.astype(BF16)
            rope(y, r, HEAD_DIM ** -0.5, put)

    def send_kv(l, r, far):
        for d in range(1, far + 1):
            @pl.when(chip + d < CHIPS)
            def _(d=d):
                kv_remote(l, r, d).start()

    def attention(j):
        l = j // ROWS
        r = j % ROWS
        for d in range(1, CHIPS):
            @pl.when((chip - d >= 0) & (d <= 2 + l))
            def _(d=d):
                kv_remote(l, r, d).wait_recv()
        lo = jnp.where(l == 1, 0, jnp.maximum(chip - 2, 0))
        count = chip - lo + 1
        reach = WINDOW + l * 1000000

        def kv_head(kh, carry):
            kcol = pl.multiple_of(kh * 256, 256)
            vcol = pl.multiple_of(HKV + kh * 256, 256)

            def score(t, sums):
                b = lo + t
                k = kvbuf[l, r, b, :, pl.ds(kcol, 256)]
                new = []
                masks = []
                for c in range(2):
                    qp = tab[c, r, 2]
                    parts = []
                    for kc in range(2):
                        off = qp - posbuf[2 * b + kc, pl.ds(r, 1), :]
                        parts.append((off >= 0.0) & (off < reach.astype(F32)))
                    masks.append(parts)
                for hh in range(2):
                    q = qbuf[r, 2 * kh + hh]
                    s = lax.dot_general(q, k, (((1,), (1,)), ((), ())), preferred_element_type=F32)
                    e = jnp.exp2(EXP2_CAP * jnp.tanh(s * (1.0 / SOFT_CAP)))
                    out = []
                    for c in range(2):
                        tot = None
                        for kc in range(2):
                            piece = jnp.where(masks[c][kc], e[c * TOK:(c + 1) * TOK, kc * 128:(kc + 1) * 128], 0.0)
                            ebuf[hh, t, c * TOK:(c + 1) * TOK, kc * 128:(kc + 1) * 128] = piece
                            tot = piece if tot is None else tot + piece
                        out.append(tot)
                    new.append(sums[hh] + jnp.concatenate(out, axis=0))
                return tuple(new)

            zero = jnp.zeros((CTOK, 128), F32)
            sums = lax.fori_loop(0, count, score, (zero, zero))
            inv = [1.0 / jnp.sum(s, axis=-1, keepdims=True) for s in sums]

            def mix(t, accs):
                v = kvbuf[l, r, lo + t, :, pl.ds(vcol, 256)]
                return tuple(accs[hh] + dot((ebuf[hh, t] * inv[hh]).astype(BF16), v) for hh in range(2))

            z2 = jnp.zeros((CTOK, HEAD_DIM), F32)
            accs = lax.fori_loop(0, count, mix, (z2, z2))
            for hh in range(2):
                col = pl.multiple_of(core * HQ + (2 * kh + hh) * 256, 256)
                obuf[:, pl.ds(col, 256)] = accs[hh].astype(BF16)
            return carry

        lax.fori_loop(0, 2, kv_head, 0)
        o_remote().start()

    def out_proj(slot):
        o_remote().wait()
        wait_w(slot)
        for t in range(5):
            col = pl.multiple_of(core * DH + t * 256, 256)
            abuf[:, pl.ds(col, 256)] = dot(obuf[...], unit(slot, t, 2048)).astype(BF16)
        a_remote().start()

    def mid_norm(j):
        l = j // ROWS
        r = j % ROWS
        a_remote().wait()

        def chunk(i, carry):
            rows = pl.ds(pl.multiple_of(i * 16, 16), 16)
            y = rms(abuf[rows, :].astype(F32), norms[pl.ds(4 * l + 1, 1), :])
            x1 = (xbuf[r, rows, :].astype(F32) + y.astype(F32)).astype(BF16)
            xbuf[r, rows, :] = x1
            mbuf[rows, :] = rms(x1.astype(F32), norms[pl.ds(4 * l + 2, 1), :])
            return carry
        lax.fori_loop(0, CTOK // 16, chunk, 0)

    def end_norm(j, par):
        l = j // ROWS
        r = j % ROWS
        d_remote(par).wait()

        def chunk(i, carry):
            rows = pl.ds(pl.multiple_of(i * 16, 16), 16)
            y = rms(dbuf[par, rows, :].astype(F32), norms[pl.ds(4 * l + 3, 1), :])
            x2 = (xbuf[r, rows, :].astype(F32) + y.astype(F32)).astype(BF16)
            xbuf[r, rows, :] = x2
            mbuf[rows, :] = rms(x2.astype(F32), norms[4:5, :])
            return carry
        lax.fori_loop(0, CTOK // 16, chunk, 0)

    def put_out(j):
        r = j % ROWS
        return pltpu.make_async_copy(
            xbuf.at[r, pl.ds(pl.multiple_of(core * TOK, TOK), TOK), :], out_hbm.at[r], out_sem.at[r])

    start_kv(wk0, wv0, 0)
    start_q(wq0, 1)
    start_wo(me >= 0, 2)
    for r in range(ROWS):
        x_local(r).start()
    tab_local().start()
    pos_local().start()
    barrier = pltpu.get_barrier_semaphore()
    for k in range(1, 8):
        pl.semaphore_signal(barrier, inc=1, device_id=at(lax.rem(me + k, 8)), device_id_type=MESH)
    pl.semaphore_wait(barrier, 7)
    x_remote(0).start()
    tab_remote().start()
    for r in range(1, ROWS):
        x_remote(r).start()
    for k in range(1, 8):
        pos_remote(k).start()

    def first_norm(r, carry):
        x_local(r).wait()
        x_remote(r).wait()

        def chunk(i, carry):
            rows = pl.ds(pl.multiple_of(i * 16, 16), 16)
            hbuf[0, rows, pl.ds(pl.multiple_of(r * DIM, DIM), DIM)] = rms(
                xbuf[r, rows, :].astype(F32), norms[0:1, :])
            return carry
        lax.fori_loop(0, CTOK // 16, chunk, 0)
        return carry

    start_gu(me >= 0, 0, 3)
    tab_local().wait()
    tab_remote().wait()
    wait_w(0)

    def a0(r):
        return hbuf[0, :, pl.ds(pl.multiple_of(r * DIM, DIM), DIM)]

    def first_kv(r, carry):
        first_norm(r, 0)
        kv_part(lambda: a0(r), 0, 0, r)
        send_kv(0, r, 2)
        return carry
    lax.fori_loop(0, ROWS, first_kv, 0)
    start_gu(me >= 0, 1, 0)
    wait_w(1)

    def first_q(r, carry):
        q_part(lambda: a0(r), 1, r)
        return carry
    lax.fori_loop(0, ROWS, first_q, 0)
    pos_local().wait()
    for k in range(1, 8):
        pos_remote(k).wait()
    start_gu(me >= 0, 2, 1)
    attention(0 * me)
    out_proj(2)

    def step(j, carry):
        first = j < ROWS
        first_next = j + 1 < ROWS
        par = j % 2
        has_qkv = (j >= 1) & (j <= ROWS)
        extra = jnp.where(has_qkv, 2, 0)
        done = jnp.where(j >= 1, jnp.minimum(j - 1, ROWS), 0)
        cb = 3 + 2 * done
        db = cb + GU + extra

        def sl(p):
            return lax.rem(p, DEPTH)

        mid_norm(j)

        def gate_up(i, carry):
            @pl.when(i + 3 < GU)
            def _():
                start_gu(first, i + 3, sl(cb + i + 3))

            @pl.when(i + 3 >= GU)
            def _():
                e = i + 3 - GU

                @pl.when(jnp.logical_not(has_qkv))
                def _():
                    start_down(first, e, sl(cb + i + 3))

                @pl.when(has_qkv & (e == 0))
                def _():
                    start_kv(wk1, wv1, sl(cb + i + 3))

                @pl.when(has_qkv & (e == 1))
                def _():
                    start_q(wq1, sl(cb + i + 3))

                @pl.when(has_qkv & (e == 2))
                def _():
                    start_down(first, 0, sl(cb + i + 3))

            @pl.when(i >= 2)
            def _():
                h_remote(par, i - 2).start()
            slot = sl(cb + i)
            wait_w(slot)
            base = core * FFH + i * 512
            prev = jnp.where(i >= 1, base - 256, base + 256)
            hbuf[par, :, pl.ds(pl.multiple_of(prev, 256), 256)] = gated(gs[...], us[...])
            g = dot(mbuf[...], unit(slot, 0))
            u = dot(mbuf[...], unit(slot, 1))
            hbuf[par, :, pl.ds(pl.multiple_of(base, 256), 256)] = gated(g, u)
            gs[...] = dot(mbuf[...], unit(slot, 2))
            us[...] = dot(mbuf[...], unit(slot, 3))
            return carry
        lax.fori_loop(0, GU, gate_up, 0)
        last = core * FFH + FFH - 256
        hbuf[par, :, pl.ds(pl.multiple_of(last, 256), 256)] = gated(gs[...], us[...])
        h_remote(par, GU - 2).start()
        h_remote(par, GU - 1).start()

        @pl.when(j >= 1)
        def _():
            end_norm(j - 1, 1 - par)

            @pl.when(has_qkv)
            def _():
                r = j - 1
                start_down(first, 1, sl(db + 1))
                wait_w(sl(cb + GU))
                kv_part(lambda: mbuf[...], sl(cb + GU), 1, r)
                send_kv(1, r, 3)
                start_down(first, 2, sl(db + 2))
                wait_w(sl(cb + GU + 1))
                q_part(lambda: mbuf[...], sl(cb + GU + 1), r)

            @pl.when(jnp.logical_not(has_qkv))
            def _():
                put_out(j - 1).start()

        @pl.when(j + 1 < STEPS)
        def _():
            attention(j + 1)

        h_all(par).wait()

        def down(n, pos):
            wait_w(sl(pos))
            col = pl.multiple_of(core * DH + n * 256, 256)
            y = dot(hbuf[par, :, 0:FFH], ring[sl(pos), 0:FFH, :]) + dot(hbuf[par, :, FFH:FF], ring[sl(pos), FFH:FF, :])
            dbuf[par, :, pl.ds(col, 256)] = y.astype(BF16)

        def down_a(n, carry):
            @pl.when(j + 1 < STEPS)
            def _():
                @pl.when(n == 0)
                def _():
                    start_wo(first_next, sl(db + 3))

                @pl.when(n >= 1)
                def _():
                    start_down(first, n + 2, sl(db + n + 3))

            @pl.when((j + 1 == STEPS) & (n <= 1))
            def _():
                start_down(first, n + 3, sl(db + n + 3))
            down(n, db + n)
            return carry
        lax.fori_loop(0, 3, down_a, 0)

        @pl.when(j + 1 < STEPS)
        def _():
            start_gu(first_next, 0, sl(db + 6))
            out_proj(sl(db + 3))

        shift = jnp.where(j + 1 < STEPS, 1, 0)

        def down_b(n, carry):
            @pl.when(j + 1 < STEPS)
            def _():
                start_gu(first_next, n - 2, sl(db + n + 4))
            down(n, db + n + shift)
            return carry
        lax.fori_loop(3, 5, down_b, 0)
        d_remote(par).start()
        return carry

    lax.fori_loop(0, STEPS, step, 0)

    end_norm(STEPS - 1 + 0 * me, (STEPS - 1) % 2)
    put_out(STEPS - 1).start()
    for r in range(ROWS):
        put_out(r).wait()
    for l in range(2):
        for r in range(ROWS):
            for d in range(1, 3 + l):
                @pl.when(chip + d < CHIPS)
                def _(l=l, r=r, d=d):
                    kv_remote(l, r, d).wait_send()


def solution(mesh):
    def device_step(hidden, positions, *weights):
        local_w = weights[:11]
        global_w = weights[11:]
        half_dim = HEAD_DIM // 2
        inv_freq = THETA ** (-(jnp.arange(half_dim, dtype=F32) * 2.0 / HEAD_DIM))
        pos = positions.astype(F32)
        angles = pos[:, :, None] * inv_freq
        tab = jnp.stack([jnp.cos(angles), jnp.sin(angles), jnp.broadcast_to(pos[:, :, None], angles.shape)], axis=1)
        pos_rows = jnp.pad(pos, ((0, 8 - ROWS), (0, 0)))
        norms = jnp.stack(local_w[7:11] + global_w[7:11])
        hbm = pl.BlockSpec(memory_space=pltpu.HBM)
        vmem = pl.BlockSpec(memory_space=pltpu.VMEM)
        dma = pltpu.SemaphoreType.DMA
        flops = 2 * ROWS * TOK * 2 * (DIM * 4096 + 2048 * DIM + 3 * DIM * FF)
        return pl.pallas_call(
            kernel,
            out_shape=jax.ShapeDtypeStruct(hidden.shape, hidden.dtype),
            in_specs=[hbm, vmem, vmem, vmem] + [hbm] * 14,
            out_specs=hbm,
            scratch_shapes=[
                pltpu.VMEM((DEPTH, FF, 256), BF16),
                pltpu.VMEM((2, ROWS, CHIPS, CTOK, 2 * HKV), BF16),
                pltpu.VMEM((ROWS, CTOK, DIM), BF16),
                pltpu.VMEM((CTOK, DIM), BF16),
                pltpu.VMEM((2, CTOK, FF), BF16),
                pltpu.VMEM((ROWS, 4, CTOK, HEAD_DIM), BF16),
                pltpu.VMEM((CTOK, 2 * HQ), BF16),
                pltpu.VMEM((CTOK, DIM), BF16),
                pltpu.VMEM((2, CTOK, DIM), BF16),
                pltpu.VMEM((2, ROWS, 3, TOK, 128), F32),
                pltpu.VMEM((8, 8, 128), F32),
                pltpu.VMEM((2, CHIPS, CTOK, CTOK), F32),
                pltpu.VMEM((CTOK, 256), F32),
                pltpu.VMEM((CTOK, 256), F32),
                dma((DEPTH,)), dma((ROWS,)), dma((ROWS,)), dma((ROWS,)),
                dma((2,)), dma((1,)), dma((8,)), dma((8,)),
                dma((2, ROWS, CHIPS)), dma((2, ROWS, CHIPS)),
                dma, dma, dma, dma,
                dma((2,)), dma((2,)), dma((2,)), dma((2,)), dma((ROWS,)),
            ],
            compiler_params=pltpu.CompilerParams(
                collective_id=0, has_side_effects=True, vmem_limit_bytes=67043328),
            cost_estimate=pl.CostEstimate(flops=flops, bytes_accessed=600000000, transcendentals=0),
            name="layers",
        )(hidden, tab, pos_rows, norms, *local_w[:7], *global_w[:7])

    specs_in = tuple([P("dp", "cp"), P("dp", "cp")] + [P()] * 22)
    return jax.shard_map(device_step, mesh=mesh, in_specs=specs_in, out_specs=P("dp", "cp"), check_vma=False)
```

```python
import functools
import math

import jax
import jax.numpy as jnp
import numpy as np
from jax import lax
from jax.experimental import pallas as pl
from jax.experimental.pallas import tpu as pltpu
from jax.sharding import PartitionSpec as P

HEAD_DIM = 256
WINDOW = 512
EPSILON = 1e-6
THETA = 10000.0
SOFT_CAP = 50.0
EXP2_CAP = SOFT_CAP * math.log2(math.e)

MESH = pl.DeviceIdType.MESH
F32 = jnp.float32
BF16 = jnp.bfloat16

ROWS = 3
TOK = 128
CTOK = 256
DIM = 2560
HQ = 1024
HKV = 512
FF = 10240
FFH = FF // 2
DH = DIM // 2
CHIPS = 4
STEPS = 2 * ROWS
DEPTH = 4
GU = FFH // 512
SCORES = 8
NCHUNK = 128
PIECE = 16
KEYS = CHIPS * CTOK


def dot(a, b):
    return jnp.dot(a, b, preferred_element_type=F32)


def rms(u, w):
    mean_sq = jnp.mean(u * u, axis=-1, keepdims=True)
    return (u * lax.rsqrt(mean_sq + EPSILON) * (1.0 + w)).astype(BF16)


def gated(g, u):
    g = g.astype(BF16).astype(F32)
    u = u.astype(BF16).astype(F32)
    return (jax.nn.gelu(g, approximate=True) * u).astype(BF16)


def kernel(x_hbm, pos_in, freq_in, n0, n1, n2, n3, n4, n5, n6, n7,
           wq0, wk0, wv0, wo0, wg0, wu0, wd0, wq1, wk1, wv1, wo1, wg1, wu1, wd1,
           out_hbm,
           ring, kvbuf, xbuf, mbuf, hown, hpeer, qbuf, obuf, abuf, dbuf, cosb, sinb, tposb, posbuf, freq, norms, r0, r1, r2, r3, r4, r5, r6, r7, ebuf, sbuf, gs, us, gb, ub,
           n_sem, ring_sem, xl_sem, xs_sem, xr_sem, ps_sem, pr_sem, kvs_sem, kvr_sem, ks_sem, kr_sem,
           os_sem, or_sem, as_sem, ar_sem, hs_sem, hr_sem, dss_sem, dr_sem, out_sem):
    me = lax.axis_index("cp")
    chip = me // 2
    core = me % 2
    peer = me + 1 - 2 * core

    def at(dev):
        return {"cp": dev}

    def start_cols(w, rows, col, slot, row0):
        pltpu.make_async_copy(
            w.at[pl.ds(0, rows), pl.ds(pl.multiple_of(col, 256), 256)],
            ring.at[slot, pl.ds(row0, rows), :], ring_sem.at[slot]).start()

    def by_layer(first, f0, f1):
        @pl.when(first)
        def _():
            f0()

        @pl.when(jnp.logical_not(first))
        def _():
            f1()

    def start_gu(first, i, slot):
        def go(wg, wu):
            col = core * FFH + i * 512
            for t in range(2):
                start_cols(wg, DIM, col + 256 * t, slot, 2 * t * DIM)
                start_cols(wu, DIM, col + 256 * t, slot, (2 * t + 1) * DIM)
        by_layer(first, lambda: go(wg0, wu0), lambda: go(wg1, wu1))

    def start_down(first, n, slot):
        def go(wd):
            start_cols(wd, FF, core * DH + n * 256, slot, 0)
        by_layer(first, lambda: go(wd0), lambda: go(wd1))

    def start_wo(first, slot):
        def go(wo):
            for t in range(5):
                start_cols(wo, 2048, core * DH + t * 256, slot, t * 2048)
        by_layer(first, lambda: go(wo0), lambda: go(wo1))

    def start_kv(wk, wv, slot):
        for t in range(2):
            start_cols(wk, DIM, core * HKV + t * 256, slot, t * DIM)
            start_cols(wv, DIM, core * HKV + t * 256, slot, (2 + t) * DIM)

    def start_q(wq, slot):
        for t in range(4):
            start_cols(wq, DIM, core * HQ + t * 256, slot, t * DIM)

    def wait_w(slot):
        pltpu.make_async_copy(wd0.at[:, pl.ds(0, 256)], ring.at[slot], ring_sem.at[slot]).wait()

    def unit(slot, t, rows=DIM):
        return ring[slot, pl.ds(t * rows, rows), :]

    def x_local(r):
        return pltpu.make_async_copy(
            x_hbm.at[r], xbuf.at[r, pl.ds(pl.multiple_of(core * TOK, TOK), TOK), :], xl_sem.at[r])

    def x_remote(r):
        return pltpu.make_async_remote_copy(
            x_hbm.at[r], xbuf.at[r, pl.ds(pl.multiple_of(core * TOK, TOK), TOK), :],
            xs_sem.at[r], xr_sem.at[r], device_id=at(peer), device_id_type=MESH)

    def norm_copy(k, src):
        return pltpu.make_async_copy(src, nraw[k], n_sem.at[k])

    all_norms = (n0, n1, n2, n3, n4, n5, n6, n7)
    nraw = (r0, r1, r2, r3, r4, r5, r6, r7)

    def freq_copy():
        return pltpu.make_async_copy(freq_in, freq, n_sem.at[8])

    def tables(c):
        rows = posbuf[2 * chip + c].astype(F32)
        cols = jnp.transpose(jnp.concatenate([rows, jnp.zeros((TOK - ROWS, TOK), F32)], axis=0))
        for r in range(ROWS):
            col = jnp.broadcast_to(cols[:, r:r + 1], (TOK, 128))
            tposb[c, r] = col.astype(jnp.int32)
            angle = col * freq[...]
            cosb[c, r] = jnp.cos(angle)
            sinb[c, r] = jnp.sin(angle)

    def pos_local():
        return pltpu.make_async_copy(pos_in, posbuf.at[me], ps_sem.at[0])

    def pos_remote(k):
        return pltpu.make_async_remote_copy(
            pos_in, posbuf.at[me], ps_sem.at[k], pr_sem.at[k],
            device_id=at(lax.rem(me + k, 8)), device_id_type=MESH)

    def kv_own(l, r):
        return kvbuf.at[l, r, pl.ds(pl.multiple_of(chip * CTOK, CTOK), CTOK), :]

    def kv_remote(l, r, d):
        return pltpu.make_async_remote_copy(
            kv_own(l, r), kv_own(l, r), kvs_sem.at[l, r, d], kvr_sem.at[l, r, d],
            device_id=at(lax.rem(me + 2 * d, 8)), device_id_type=MESH)

    def kv_piece(r, h):
        return kvbuf.at[0, r, pl.ds(pl.multiple_of(CTOK + h * TOK, TOK), TOK), :]

    def kv_second(r, h):
        return pltpu.make_async_remote_copy(
            kv_piece(r, h), kv_piece(r, h), ks_sem.at[r, h], kr_sem.at[r, h],
            device_id=at(6 + core), device_id_type=MESH)

    def kv_relay(r, h):
        return pltpu.make_async_remote_copy(
            kv_piece(r, h), kv_piece(r, h), ks_sem.at[r, h], kr_sem.at[r, h],
            device_id=at(4 + core), device_id_type=MESH)

    def forward(r, h):
        @pl.when(chip == 3)
        def _():
            kv_second(r, h).wait_recv()
            kv_relay(r, h).start()

    def send_kv0(r):
        @pl.when(chip == 0)
        def _():
            kv_remote(0, r, 2).start()
            kv_remote(0, r, 1).start()

        @pl.when(chip == 1)
        def _():
            for h in range(2):
                kv_second(r, h).start()

        @pl.when(chip == 2)
        def _():
            kv_remote(0, r, 1).start()

    def half(buf, width):
        return buf.at[:, pl.ds(pl.multiple_of(core * width, 256), width)]

    def o_remote():
        return pltpu.make_async_remote_copy(
            half(obuf, HQ), half(obuf, HQ), os_sem, or_sem, device_id=at(peer), device_id_type=MESH)

    def a_remote():
        return pltpu.make_async_remote_copy(
            half(abuf, DH), half(abuf, DH), as_sem, ar_sem, device_id=at(peer), device_id_type=MESH)

    def d_remote(par):
        return pltpu.make_async_remote_copy(
            half(dbuf.at[par], DH), half(dbuf.at[par], DH), dss_sem.at[par], dr_sem.at[par],
            device_id=at(peer), device_id_type=MESH)

    def h_remote(par, i):
        cols = pl.ds(pl.multiple_of(i * 512, 512), 512)
        return pltpu.make_async_remote_copy(
            hown.at[:, cols], hpeer.at[par, :, cols], hs_sem.at[par], hr_sem.at[par],
            device_id=at(peer), device_id_type=MESH)

    def h_all(par):
        return pltpu.make_async_remote_copy(
            hown, hpeer.at[par], hs_sem.at[par], hr_sem.at[par], device_id=at(peer), device_id_type=MESH)

    def rope(y, r, t, dst):
        y = y.astype(BF16).astype(F32)
        for c in range(2):
            f = y[c * TOK:(c + 1) * TOK, :128]
            s = y[c * TOK:(c + 1) * TOK, 128:]
            cos = cosb[c, r]
            sin = sinb[c, r]
            dst(c, (f * cos - s * sin) * t, (s * cos + f * sin) * t)

    def kv_part(src, slot, l, r):
        for t in range(2):
            y = dot(src(), unit(slot, t))

            def put(c, a, b, t=t):
                rows = pl.ds(pl.multiple_of(chip * CTOK + c * TOK, TOK), TOK)
                kvbuf[l, r, rows, t * 256:t * 256 + 128] = a.astype(BF16)
                kvbuf[l, r, rows, t * 256 + 128:t * 256 + 256] = b.astype(BF16)
            rope(y, r, 1.0, put)
            kvbuf[l, r, pl.ds(pl.multiple_of(chip * CTOK, CTOK), CTOK), HKV + t * 256:HKV + t * 256 + 256] = dot(src(), unit(slot, 2 + t)).astype(BF16)

    def q_part(src, slot, r):
        for t in range(4):
            y = dot(src(), unit(slot, t))

            def put(c, a, b, t=t):
                rows = pl.ds(c * TOK, TOK)
                qbuf[r, t, rows, 0:128] = a.astype(BF16)
                qbuf[r, t, rows, 128:256] = b.astype(BF16)
            rope(y, r, HEAD_DIM ** -0.5, put)

    def send_kv(l, r, far):
        for d in range(1, far + 1):
            @pl.when(chip + d < CHIPS)
            def _(d=d):
                kv_remote(l, r, d).start()

    def kv_wait(j):
        l = j // ROWS
        r = j % ROWS
        for d in range(1, CHIPS):
            @pl.when((chip - d >= 0) & (l == 1))
            def _(d=d):
                kv_remote(1, r, d).wait_recv()

        @pl.when(l == 0)
        def _():
            @pl.when((chip == 1) | (chip == 3))
            def _():
                kv_remote(0, r, 1).wait_recv()

            @pl.when(chip == 2)
            def _():
                kv_remote(0, r, 2).wait_recv()
                for h in range(2):
                    kv_relay(r, h).wait_recv()

    def score(j, kh, t):
        l = j // ROWS
        r = j % ROWS
        reach = WINDOW + l * 1000000
        k = kvbuf[l, r, pl.ds(pl.multiple_of(t * CTOK, CTOK), CTOK), pl.ds(pl.multiple_of(kh * 256, 256), 256)]
        masks = {}
        for c in range(2):
            for kc in range(2):
                off = tposb[c, r] - posbuf[2 * t + kc, pl.ds(r, 1), :]
                masks[c, kc] = (off >= 0) & (off < reach)
        for hh in range(2):
            q = qbuf[r, 2 * kh + hh]
            s = lax.dot_general(q, k, (((1,), (1,)), ((), ())), preferred_element_type=F32)
            e = jnp.exp2(EXP2_CAP * jnp.tanh(s * (1.0 / SOFT_CAP)))
            for c in range(2):
                rows = slice(c * TOK, (c + 1) * TOK)
                tot = jnp.where(t == 0, 0.0, sbuf[2 * kh + hh, rows, :])
                for kc in range(2):
                    piece = jnp.where(masks[c, kc], e[rows, kc * 128:(kc + 1) * 128], 0.0)
                    ebuf[2 * kh + hh, rows, pl.ds(pl.multiple_of(t * CTOK + kc * 128, 128), 128)] = piece
                    tot = tot + piece
                sbuf[2 * kh + hh, rows, :] = tot

    def mix(j, kh):
        l = j // ROWS
        r = j % ROWS
        v = kvbuf[l, r, :, pl.ds(pl.multiple_of(HKV + kh * 256, 256), 256)]
        for hh in range(2):
            inv = 1.0 / jnp.sum(sbuf[2 * kh + hh], axis=-1, keepdims=True)
            p = (ebuf[2 * kh + hh] * inv).astype(BF16)
            col = pl.multiple_of(core * HQ + (2 * kh + hh) * 256, 256)
            obuf[:, pl.ds(col, 256)] = dot(p, v).astype(BF16)

    def attention(j):
        with jax.named_scope("att_wait"):
            forward(0, 1)
            kv_wait(j)
        with jax.named_scope("att"):
            def go(i, carry):
                score(j, i // CHIPS, i % CHIPS)
                return carry
            lax.fori_loop(0, SCORES, go, 0)

            def go2(i, carry):
                mix(j, i)
                return carry
            lax.fori_loop(0, 2, go2, 0)
        o_remote().start()

    def out_proj(slot):
        with jax.named_scope("o_wait"):
            o_remote().wait()
        with jax.named_scope("wo_wait"):
            wait_w(slot)
        for t in range(5):
            col = pl.multiple_of(core * DH + t * 256, 256)
            abuf[:, pl.ds(col, 256)] = dot(obuf[...], unit(slot, t, 2048)).astype(BF16)
        a_remote().start()

    def mid_rows(j, base, keep=None):
        l = j // ROWS
        r = j % ROWS
        for t in range(0, NCHUNK, PIECE):
            rows = pl.ds(pl.multiple_of(base + t, PIECE), PIECE)
            y = rms(abuf[rows, :].astype(F32), norms[4 * l + 1])
            x = xbuf[r, rows, :]
            x1 = (x.astype(F32) + y.astype(F32)).astype(BF16)
            xbuf[r, rows, :] = x1 if keep is None else jnp.where(keep, x1, x)
            mbuf[rows, :] = rms(x1.astype(F32), norms[4 * l + 2])

    def end_rows(j, par, base, keep=None):
        l = j // ROWS
        r = j % ROWS
        for t in range(0, NCHUNK, PIECE):
            rows = pl.ds(pl.multiple_of(base + t, PIECE), PIECE)
            y = rms(dbuf[par, rows, :].astype(F32), norms[4 * l + 3])
            x = xbuf[r, rows, :]
            x2 = (x.astype(F32) + y.astype(F32)).astype(BF16)
            xbuf[r, rows, :] = x2 if keep is None else jnp.where(keep, x2, x)
            dbuf[par, rows, :] = rms(x2.astype(F32), norms[4])

    def put_out(j):
        r = j % ROWS
        return pltpu.make_async_copy(
            xbuf.at[r, pl.ds(pl.multiple_of(core * TOK, TOK), TOK), :], out_hbm.at[r], out_sem.at[r])

    pos_local().start()
    x_local(0).start()
    freq_copy().start()
    for k in range(8):
        norm_copy(k, all_norms[k]).start()
    x_local(1).start()
    x_local(2).start()
    def clear(i, carry):
        l = i // (ROWS * CHIPS)
        r = (i // CHIPS) % ROWS
        b = i % CHIPS

        @pl.when((b > chip) | ((l == 0) & (b < chip - 2)))
        def _():
            kvbuf[l, r, pl.ds(pl.multiple_of(b * CTOK, CTOK), CTOK), HKV:] = jnp.zeros((CTOK, HKV), BF16)
        return carry
    lax.fori_loop(0, 2 * ROWS * CHIPS, clear, 0)
    freq_copy().wait()
    pos_local().wait()
    start_kv(wk0, wv0, 0)
    with jax.named_scope("tables"):
        tables(core)
    barrier = pltpu.get_barrier_semaphore()
    for k in range(1, 8):
        pl.semaphore_signal(barrier, inc=1, device_id=at(lax.rem(me + k, 8)), device_id_type=MESH)
    with jax.named_scope("entry"):
        pl.semaphore_wait(barrier, 7)
    x_remote(0).start()
    for k in range(1, 8):
        pos_remote(k).start()
    for r in range(1, ROWS):
        x_remote(r).start()
    for k in range(8):
        norm_copy(k, all_norms[k]).wait()
    for k in range(8):
        norms[k] = nraw[k][...].reshape(1, DIM)

    @pl.when(core == 0)
    def _():
        pos_remote(7).wait_recv()

    @pl.when(core == 1)
    def _():
        pos_remote(1).wait_recv()
    with jax.named_scope("tables"):
        tables(1 - core)
    start_q(wq0, 1)
    start_wo(me >= 0, 2)

    def first_norm(r, carry):
        with jax.named_scope("x_wait"):
            x_local(r).wait()
            x_remote(r).wait()

        def chunk(i, carry):
            for t in range(0, NCHUNK, PIECE):
                rows = pl.ds(pl.multiple_of(i * NCHUNK + t, PIECE), PIECE)
                hpeer[r // 2, rows, pl.ds(pl.multiple_of((r % 2) * DIM, DIM), DIM)] = rms(
                    xbuf[r, rows, :].astype(F32), norms[0])
            return carry
        lax.fori_loop(0, CTOK // NCHUNK, chunk, 0)
        return carry

    start_gu(me >= 0, 0, 3)
    wait_w(0)

    def a0(r):
        return hpeer[r // 2, :, pl.ds(pl.multiple_of((r % 2) * DIM, DIM), DIM)]

    def first_kv(r, carry):
        first_norm(r, 0)
        kv_part(lambda: a0(r), 0, 0, r)
        send_kv0(r)
        return carry
    with jax.named_scope("first_kv"):
        lax.fori_loop(0, ROWS, first_kv, 0)
    start_gu(me >= 0, 1, 0)
    wait_w(1)

    def first_q(r, carry):
        q_part(lambda: a0(r), 1, r)

        @pl.when(r == 1)
        def _():
            forward(0, 0)
        return carry
    with jax.named_scope("first_q"):
        lax.fori_loop(0, ROWS, first_q, 0)
    start_gu(me >= 0, 2, 1)
    for k in range(1, 8):
        pos_remote(k).wait_send()

    @pl.when(core == 0)
    def _():
        for k in range(1, 7):
            pos_remote(k).wait_recv()

    @pl.when(core == 1)
    def _():
        for k in range(2, 8):
            pos_remote(k).wait_recv()
    attention(0 * me)
    forward(1, 0)
    out_proj(2)
    with jax.named_scope("a_wait"):
        a_remote().wait()

    def first_mid(i, carry):
        mid_rows(0 * me, i * NCHUNK)
        return carry
    lax.fori_loop(0, CTOK // NCHUNK, first_mid, 0)

    def step(j, carry):
        first = j < ROWS
        first_next = j + 1 < ROWS
        more = j + 1 < STEPS
        par = j % 2
        has_qkv = (j >= 1) & (j <= ROWS)
        next_qkv = j + 1 <= ROWS
        done = jnp.where(j >= 1, jnp.minimum(j - 1, ROWS), 0)
        extra = jnp.where(has_qkv, 2, 0)
        sb = 3 + 2 * done
        db = sb + extra + GU
        nxt = jnp.minimum(j + 1, STEPS - 1)

        def sl(p):
            return lax.rem(p, DEPTH)

        def gate_up(i, pos, beside):
            slot = sl(pos)
            with jax.named_scope("gu_wait"):
                wait_w(slot)
            base = i * 512
            prev = base - 256 if not isinstance(i, int) or i > 0 else base + 256
            hown[:, pl.ds(pl.multiple_of(prev, 256), 256)] = gated(gs[...], us[...])
            g = dot(mbuf[...], unit(slot, 0))
            u = dot(mbuf[...], unit(slot, 1))
            beside()
            hown[:, pl.ds(pl.multiple_of(base, 256), 256)] = gated(g, u)
            gs[...] = dot(mbuf[...], unit(slot, 2))
            us[...] = dot(mbuf[...], unit(slot, 3))

        @pl.when(has_qkv)
        def _():
            start_q(wq1, sl(sb + 3))

        @pl.when(jnp.logical_not(has_qkv))
        def _():
            start_gu(first, 3, sl(sb + 3))
        with jax.named_scope("gate_up0"):
            gate_up(0, sb, lambda: None)

        @pl.when(has_qkv)
        def _():
            start_gu(first, 2, sl(sb + 4))

        @pl.when(jnp.logical_not(has_qkv))
        def _():
            start_gu(first, 4, sl(sb + 4))

        @pl.when(j >= 1)
        def _():
            with jax.named_scope("d_wait"):
                d_remote(1 - par).wait()
        last = jnp.maximum(j - 1, 0)

        def ending():
            for c in range(2):
                end_rows(last, 1 - par, c * NCHUNK, j >= 1)
        with jax.named_scope("gate_up1"):
            gate_up(1, sb + 1, ending)

        @pl.when(has_qkv)
        def _():
            start_gu(first, 3, sl(sb + 5))
            wait_w(sl(sb + 2))
            with jax.named_scope("kv"):
                kv_part(lambda: dbuf[1 - par], sl(sb + 2), 1, last)
            send_kv(1, last, 3)
            start_gu(first, 4, sl(sb + 6))
            wait_w(sl(sb + 3))
            with jax.named_scope("q"):
                q_part(lambda: dbuf[1 - par], sl(sb + 3), last)

        @pl.when(j > ROWS)
        def _():
            put_out(j - 1).start()

        @pl.when(more)
        def _():
            with jax.named_scope("att_wait"):
                @pl.when(j == 0)
                def _():
                    forward(1, 1)

                @pl.when(j == 1)
                def _():
                    forward(2, 1)
                kv_wait(j + 1)

        def scoring(i, carry):
            pos = sb + extra + i

            @pl.when(i + 3 < GU)
            def _():
                start_gu(first, i + 3, sl(pos + 3))

            @pl.when(i + 3 >= GU)
            def _():
                start_down(first, i + 3 - GU, sl(pos + 3))
            h_remote(par, i - 2).start()
            e = i - 2
            gate_up(i, pos, lambda: score(nxt, e // CHIPS, e % CHIPS))
            return carry
        with jax.named_scope("gate_up"):
            lax.fori_loop(2, GU, scoring, 0)

        hown[:, FFH - 256:FFH] = gated(gs[...], us[...])
        h_remote(par, GU - 2).start()
        h_remote(par, GU - 1).start()

        @pl.when(j == 0)
        def _():
            forward(2, 0)

        def down_col(n):
            return pl.ds(pl.multiple_of(core * DH + n * 256, 256), 256)

        mine = pl.ds(pl.multiple_of(core * FFH, FFH), FFH)
        other = pl.ds(pl.multiple_of((1 - core) * FFH, FFH), FFH)
        with jax.named_scope("down_a"):
            @pl.when(more)
            def _():
                start_wo(first_next, sl(db + 3))

            @pl.when(jnp.logical_not(more))
            def _():
                start_down(first, 3, sl(db + 3))
            wait_w(sl(db))
            wait_w(sl(db + 1))
            gs[...] = dot(hown[...], ring[sl(db), mine, :])
            mix(nxt, 0)
            us[...] = dot(hown[...], ring[sl(db + 1), mine, :])
            mix(nxt, 1)

            @pl.when(more)
            def _():
                o_remote().start()
            with jax.named_scope("h_wait"):
                h_all(par).wait()
            gb[...] = dot(hpeer[par], ring[sl(db), other, :])
            ub[...] = dot(hpeer[par], ring[sl(db + 1), other, :])
            dbuf[par, :, down_col(0)] = (gs[...] + gb[...]).astype(BF16)
            dbuf[par, :, down_col(1)] = (us[...] + ub[...]).astype(BF16)

        @pl.when(more)
        def _():
            start_down(first, 3, sl(db + 4))
            start_down(first, 4, sl(db + 5))

        @pl.when(jnp.logical_not(more))
        def _():
            start_down(first, 4, sl(db + 4))
        with jax.named_scope("down2"):
            wait_w(sl(db + 2))
            gs[...] = dot(hown[...], ring[sl(db + 2), mine, :])
            us[...] = dot(hpeer[par], ring[sl(db + 2), other, :])
            dbuf[par, :, down_col(2)] = (gs[...] + us[...]).astype(BF16)

        @pl.when(more)
        def _():
            start_gu(first_next, 0, sl(db + 6))
            with jax.named_scope("proj"):
                out_proj(sl(db + 3))
            start_gu(first_next, 1, sl(db + 7))
        s3 = sl(db + 3 + jnp.where(more, 1, 0))
        s4 = sl(db + 4 + jnp.where(more, 1, 0))
        with jax.named_scope("down3"):
            wait_w(s3)
            wait_w(s4)
            gs[...] = dot(hown[...], ring[s3, mine, :])
            us[...] = dot(hown[...], ring[s4, mine, :])

        @pl.when(more)
        def _():
            with jax.named_scope("a_wait"):
                a_remote().wait()

        with jax.named_scope("down4"):
            gb[...] = dot(hpeer[par], ring[s3, other, :])
            ub[...] = dot(hpeer[par], ring[s4, other, :])
            for c in range(2):
                mid_rows(nxt, c * NCHUNK, more)
            dbuf[par, :, down_col(3)] = (gs[...] + gb[...]).astype(BF16)
            dbuf[par, :, down_col(4)] = (us[...] + ub[...]).astype(BF16)

        @pl.when(more)
        def _():
            @pl.when(next_qkv)
            def _():
                start_kv(wk1, wv1, sl(db + 8))

            @pl.when(jnp.logical_not(next_qkv))
            def _():
                start_gu(first_next, 2, sl(db + 8))
        d_remote(par).start()
        return carry

    lax.fori_loop(0, STEPS, step, 0)

    d_remote((STEPS - 1) % 2).wait()

    def final(i, carry):
        end_rows(STEPS - 1 + 0 * me, (STEPS - 1) % 2, core * TOK + i * NCHUNK)
        return carry
    lax.fori_loop(0, TOK // NCHUNK, final, 0)
    put_out(STEPS - 1).start()
    for r in range(ROWS):
        put_out(r).wait()
    for r in range(ROWS):
        for d in range(1, CHIPS):
            @pl.when(chip + d < CHIPS)
            def _(r=r, d=d):
                kv_remote(1, r, d).wait_send()

        @pl.when(chip == 0)
        def _(r=r):
            kv_remote(0, r, 2).wait_send()

        @pl.when((chip == 0) | (chip == 2))
        def _(r=r):
            kv_remote(0, r, 1).wait_send()

        @pl.when(chip == 1)
        def _(r=r):
            for h in range(2):
                kv_second(r, h).wait_send()

        @pl.when(chip == 3)
        def _(r=r):
            for h in range(2):
                kv_relay(r, h).wait_send()


def solution(mesh):
    def device_step(hidden, positions, *weights):
        local_w = weights[:11]
        global_w = weights[11:]
        half_dim = HEAD_DIM // 2
        inv_freq = (THETA ** (-(np.arange(half_dim, dtype=np.float64) * 2.0 / HEAD_DIM))).astype(np.float32)
        freq = jnp.asarray(inv_freq.reshape(1, half_dim))
        norms = local_w[7:11] + global_w[7:11]
        hbm = pl.BlockSpec(memory_space=pltpu.HBM)
        dma = pltpu.SemaphoreType.DMA
        flops = 2 * ROWS * TOK * 2 * (DIM * 4096 + 2048 * DIM + 3 * DIM * FF)
        return pl.pallas_call(
            kernel,
            out_shape=jax.ShapeDtypeStruct(hidden.shape, hidden.dtype),
            in_specs=[hbm] * 25,
            out_specs=hbm,
            scratch_shapes=[
                pltpu.VMEM((DEPTH, FF, 256), BF16),
                pltpu.VMEM((2, ROWS, KEYS, 2 * HKV), BF16),
                pltpu.VMEM((ROWS, CTOK, DIM), BF16),
                pltpu.VMEM((CTOK, DIM), BF16),
                pltpu.VMEM((CTOK, FFH), BF16),
                pltpu.VMEM((2, CTOK, FFH), BF16),
                pltpu.VMEM((ROWS, 4, CTOK, HEAD_DIM), BF16),
                pltpu.VMEM((CTOK, 2 * HQ), BF16),
                pltpu.VMEM((CTOK, DIM), BF16),
                pltpu.VMEM((2, CTOK, DIM), BF16),
                pltpu.VMEM((2, ROWS, TOK, 128), F32),
                pltpu.VMEM((2, ROWS, TOK, 128), F32),
                pltpu.VMEM((2, ROWS, TOK, 128), jnp.int32),
                pltpu.VMEM((8, ROWS, 128), jnp.int32),
                pltpu.VMEM((1, 128), F32),
                pltpu.VMEM((8, 1, DIM), F32),
                *[pltpu.VMEM((DIM,), F32)] * 8,
                pltpu.VMEM((4, CTOK, KEYS), F32),
                pltpu.VMEM((4, CTOK, 128), F32),
                *[pltpu.VMEM((CTOK, 256), F32)] * 4,
                dma((9,)), dma((DEPTH,)), dma((ROWS,)), dma((ROWS,)), dma((ROWS,)),
                dma((8,)), dma((8,)),
                dma((2, ROWS, CHIPS)), dma((2, ROWS, CHIPS)), dma((ROWS, 2)), dma((ROWS, 2)),
                dma, dma, dma, dma,
                dma((2,)), dma((2,)), dma((2,)), dma((2,)), dma((ROWS,)),
            ],
            compiler_params=pltpu.CompilerParams(
                collective_id=0, has_side_effects=True, vmem_limit_bytes=67043328),
            cost_estimate=pl.CostEstimate(flops=flops, bytes_accessed=600000000, transcendentals=0),
            name="layers",
        )(hidden, positions, freq, *norms, *local_w[:7], *global_w[:7])

    specs_in = tuple([P("dp", "cp"), P("dp", "cp")] + [P()] * 22)
    return jax.shard_map(device_step, mesh=mesh, in_specs=specs_in, out_specs=P("dp", "cp"), check_vma=False)
```

```python
import functools
import math

import jax
import jax.numpy as jnp
import numpy as np
from jax import lax
from jax.experimental import pallas as pl
from jax.experimental.pallas import tpu as pltpu
from jax.sharding import PartitionSpec as P

HEAD_DIM = 256
WINDOW = 512
EPSILON = 1e-6
THETA = 10000.0
SOFT_CAP = 50.0
EXP2_CAP = SOFT_CAP * math.log2(math.e)

MESH = pl.DeviceIdType.MESH
F32 = jnp.float32
BF16 = jnp.bfloat16

ROWS = 3
TOK = 128
CTOK = 256
DIM = 2560
HQ = 1024
HKV = 512
FF = 10240
FFH = FF // 2
DH = DIM // 2
CHIPS = 4
STEPS = 2 * ROWS
DEPTH = 4
GU = FFH // 512
SCORES = 8
NCHUNK = 128
PIECE = 16
PIECES = 4
PTOK = CTOK // PIECES
KEYS = CHIPS * CTOK


def dot(a, b):
    return jnp.dot(a, b, preferred_element_type=F32)


def rms(u, w):
    mean_sq = jnp.mean(u * u, axis=-1, keepdims=True)
    return (u * lax.rsqrt(mean_sq + EPSILON) * (1.0 + w)).astype(BF16)


def gated(g, u):
    g = g.astype(BF16).astype(F32)
    u = u.astype(BF16).astype(F32)
    return (jax.nn.gelu(g, approximate=True) * u).astype(BF16)


def kernel(x_hbm, pos_in, freq_in, n0, n1, n2, n3, n4, n5, n6, n7,
           wq0, wk0, wv0, wo0, wg0, wu0, wd0, wq1, wk1, wv1, wo1, wg1, wu1, wd1,
           out_hbm,
           ring, kvbuf, xbuf, mbuf, hown, hpeer, qbuf, obuf, abuf, dbuf, cosb, sinb, tposb, posbuf, freq, norms, r0, r1, r2, r3, r4, r5, r6, r7, ebuf, sbuf, gs, us, gb, ub,
           n_sem, ring_sem, half_sem, xl_sem, xs_sem, xr_sem, ps_sem, pr_sem, kvs_sem, kvr_sem, ks_sem, kr_sem,
           os_sem, or_sem, as_sem, ar_sem, hs_sem, hr_sem, dss_sem, dr_sem, out_sem):
    me = lax.axis_index("cp")
    chip = me // 2
    core = me % 2
    peer = me + 1 - 2 * core

    def at(dev):
        return {"cp": dev}

    def start_cols(w, rows, col, slot, row0):
        pltpu.make_async_copy(
            w.at[pl.ds(0, rows), pl.ds(pl.multiple_of(col, 256), 256)],
            ring.at[slot, pl.ds(row0, rows), :], ring_sem.at[slot]).start()

    def by_layer(first, f0, f1):
        @pl.when(first)
        def _():
            f0()

        @pl.when(jnp.logical_not(first))
        def _():
            f1()

    def start_gu(first, i, slot):
        def go(wg, wu):
            col = core * FFH + i * 512
            for t in range(2):
                start_cols(wg, DIM, col + 256 * t, slot, 2 * t * DIM)
                start_cols(wu, DIM, col + 256 * t, slot, (2 * t + 1) * DIM)
        by_layer(first, lambda: go(wg0, wu0), lambda: go(wg1, wu1))

    def start_down(first, n, slot):
        def go(wd):
            start_cols(wd, FF, core * DH + n * 256, slot, 0)
        by_layer(first, lambda: go(wd0), lambda: go(wd1))

    def start_wo(first, slot):
        def go(wo):
            for t in range(5):
                start_cols(wo, 2048, core * DH + t * 256, slot, t * 2048)
        by_layer(first, lambda: go(wo0), lambda: go(wo1))

    def start_kv(wk, wv, slot):
        for t in range(2):
            start_cols(wk, DIM, core * HKV + t * 256, slot, t * DIM)
            start_cols(wv, DIM, core * HKV + t * 256, slot, (2 + t) * DIM)

    def start_q(wq, slot):
        for t in range(4):
            start_cols(wq, DIM, core * HQ + t * 256, slot, t * DIM)

    def wait_w(slot):
        pltpu.make_async_copy(wd0.at[:, pl.ds(0, 256)], ring.at[slot], ring_sem.at[slot]).wait()

    def unit(slot, t, rows=DIM):
        return ring[slot, pl.ds(t * rows, rows), :]

    def x_local(r):
        return pltpu.make_async_copy(
            x_hbm.at[r], xbuf.at[r, pl.ds(pl.multiple_of(core * TOK, TOK), TOK), :], xl_sem.at[r])

    def x_remote(r):
        return pltpu.make_async_remote_copy(
            x_hbm.at[r], xbuf.at[r, pl.ds(pl.multiple_of(core * TOK, TOK), TOK), :],
            xs_sem.at[r], xr_sem.at[r], device_id=at(peer), device_id_type=MESH)

    def norm_copy(k, src):
        return pltpu.make_async_copy(src, nraw[k], n_sem.at[k])

    all_norms = (n0, n1, n2, n3, n4, n5, n6, n7)
    nraw = (r0, r1, r2, r3, r4, r5, r6, r7)

    def freq_copy():
        return pltpu.make_async_copy(freq_in, freq, n_sem.at[8])

    def tables(c):
        rows = posbuf[2 * chip + c].astype(F32)
        cols = jnp.transpose(jnp.concatenate([rows, jnp.zeros((TOK - ROWS, TOK), F32)], axis=0))
        for r in range(ROWS):
            col = jnp.broadcast_to(cols[:, r:r + 1], (TOK, 128))
            tposb[c, r] = col.astype(jnp.int32)
            angle = col * freq[...]
            cosb[c, r] = jnp.cos(angle)
            sinb[c, r] = jnp.sin(angle)

    def pos_local():
        return pltpu.make_async_copy(pos_in, posbuf.at[me], ps_sem.at[0])

    def pos_remote(k):
        return pltpu.make_async_remote_copy(
            pos_in, posbuf.at[me], ps_sem.at[k], pr_sem.at[k],
            device_id=at(lax.rem(me + k, 8)), device_id_type=MESH)

    def kv_own(l, r):
        return kvbuf.at[l, r, pl.ds(pl.multiple_of(chip * CTOK, CTOK), CTOK), :]

    def kv_remote(l, r, d):
        return pltpu.make_async_remote_copy(
            kv_own(l, r), kv_own(l, r), kvs_sem.at[l, r, d], kvr_sem.at[l, r, d],
            device_id=at(lax.rem(me + 2 * d, 8)), device_id_type=MESH)

    def kv_piece(r, h):
        return kvbuf.at[0, r, pl.ds(pl.multiple_of(CTOK + h * PTOK, PTOK), PTOK), :]

    def kv_second(r, h):
        return pltpu.make_async_remote_copy(
            kv_piece(r, h), kv_piece(r, h), ks_sem.at[r, h], kr_sem.at[r, h],
            device_id=at(6 + core), device_id_type=MESH)

    def kv_relay(r, h):
        return pltpu.make_async_remote_copy(
            kv_piece(r, h), kv_piece(r, h), ks_sem.at[r, h], kr_sem.at[r, h],
            device_id=at(4 + core), device_id_type=MESH)

    def forward(r, h):
        @pl.when(chip == 3)
        def _():
            kv_second(r, h).wait_recv()
            kv_relay(r, h).start()

    def send_kv0(r):
        @pl.when(chip == 0)
        def _():
            kv_remote(0, r, 2).start()
            kv_remote(0, r, 1).start()

        @pl.when(chip == 1)
        def _():
            for h in range(PIECES):
                kv_second(r, h).start()

        @pl.when(chip == 2)
        def _():
            kv_remote(0, r, 1).start()

    def half(buf, width):
        return buf.at[:, pl.ds(pl.multiple_of(core * width, 256), width)]

    def o_remote(kh):
        cols = obuf.at[:, pl.ds(pl.multiple_of(core * HQ + kh * 512, 512), 512)]
        return pltpu.make_async_remote_copy(
            cols, cols, os_sem.at[kh], or_sem.at[kh], device_id=at(peer), device_id_type=MESH)

    def a_remote():
        return pltpu.make_async_remote_copy(
            half(abuf, DH), half(abuf, DH), as_sem, ar_sem, device_id=at(peer), device_id_type=MESH)

    def d_remote(par):
        return pltpu.make_async_remote_copy(
            half(dbuf.at[par], DH), half(dbuf.at[par], DH), dss_sem.at[par], dr_sem.at[par],
            device_id=at(peer), device_id_type=MESH)

    def h_remote(par, i):
        cols = pl.ds(pl.multiple_of(i * 512, 512), 512)
        return pltpu.make_async_remote_copy(
            hown.at[:, cols], hpeer.at[par, :, cols], hs_sem.at[par], hr_sem.at[par],
            device_id=at(peer), device_id_type=MESH)

    def h_all(par):
        return pltpu.make_async_remote_copy(
            hown, hpeer.at[par], hs_sem.at[par], hr_sem.at[par], device_id=at(peer), device_id_type=MESH)

    def rope(y, r, t, dst):
        y = y.astype(BF16).astype(F32)
        for c in range(2):
            f = y[c * TOK:(c + 1) * TOK, :128]
            s = y[c * TOK:(c + 1) * TOK, 128:]
            cos = cosb[c, r]
            sin = sinb[c, r]
            dst(c, (f * cos - s * sin) * t, (s * cos + f * sin) * t)

    def kv_part(src, slot, l, r):
        for t in range(2):
            y = dot(src(), unit(slot, t))

            def put(c, a, b, t=t):
                rows = pl.ds(pl.multiple_of(chip * CTOK + c * TOK, TOK), TOK)
                kvbuf[l, r, rows, t * 256:t * 256 + 128] = a.astype(BF16)
                kvbuf[l, r, rows, t * 256 + 128:t * 256 + 256] = b.astype(BF16)
            rope(y, r, 1.0, put)
            kvbuf[l, r, pl.ds(pl.multiple_of(chip * CTOK, CTOK), CTOK), HKV + t * 256:HKV + t * 256 + 256] = dot(src(), unit(slot, 2 + t)).astype(BF16)

    def q_part(src, slot, r):
        for t in range(4):
            y = dot(src(), unit(slot, t))

            def put(c, a, b, t=t):
                rows = pl.ds(c * TOK, TOK)
                qbuf[r, t, rows, 0:128] = a.astype(BF16)
                qbuf[r, t, rows, 128:256] = b.astype(BF16)
            rope(y, r, HEAD_DIM ** -0.5, put)

    def send_kv(l, r, far):
        for d in range(1, far + 1):
            @pl.when(chip + d < CHIPS)
            def _(d=d):
                kv_remote(l, r, d).start()

    def kv_wait(j):
        l = j // ROWS
        r = j % ROWS
        for d in range(1, CHIPS):
            @pl.when((chip - d >= 0) & (l == 1))
            def _(d=d):
                kv_remote(1, r, d).wait_recv()

        @pl.when(l == 0)
        def _():
            @pl.when((chip == 1) | (chip == 3))
            def _():
                kv_remote(0, r, 1).wait_recv()

            @pl.when(chip == 2)
            def _():
                kv_remote(0, r, 2).wait_recv()
                for h in range(PIECES):
                    kv_relay(r, h).wait_recv()

    def score(j, kh, t, fresh):
        l = j // ROWS
        r = j % ROWS
        reach = WINDOW + l * 1000000
        k = kvbuf[l, r, pl.ds(pl.multiple_of(t * CTOK, CTOK), CTOK), pl.ds(pl.multiple_of(kh * 256, 256), 256)]
        masks = {}
        for c in range(2):
            for kc in range(2):
                off = tposb[c, r] - posbuf[2 * t + kc, pl.ds(r, 1), :]
                masks[c, kc] = (off >= 0) & (off < reach)
        for hh in range(2):
            q = qbuf[r, 2 * kh + hh]
            s = lax.dot_general(q, k, (((1,), (1,)), ((), ())), preferred_element_type=F32)
            e = jnp.exp2(EXP2_CAP * jnp.tanh(s * (1.0 / SOFT_CAP)))
            for c in range(2):
                rows = slice(c * TOK, (c + 1) * TOK)
                tot = jnp.where(fresh, 0.0, sbuf[2 * kh + hh, rows, :])
                for kc in range(2):
                    piece = jnp.where(masks[c, kc], e[rows, kc * 128:(kc + 1) * 128], 0.0)
                    ebuf[2 * kh + hh, rows, pl.ds(pl.multiple_of(t * CTOK + kc * 128, 128), 128)] = piece
                    tot = tot + piece
                sbuf[2 * kh + hh, rows, :] = tot

    def mix(j, kh):
        l = j // ROWS
        r = j % ROWS
        v = kvbuf[l, r, :, pl.ds(pl.multiple_of(HKV + kh * 256, 256), 256)]
        for hh in range(2):
            inv = 1.0 / jnp.sum(sbuf[2 * kh + hh], axis=-1, keepdims=True)
            p = (ebuf[2 * kh + hh] * inv).astype(BF16)
            col = pl.multiple_of(core * HQ + (2 * kh + hh) * 256, 256)
            obuf[:, pl.ds(col, 256)] = dot(p, v).astype(BF16)

    def attention():
        zero = 0 * me

        def block(t, fresh):
            def go(kh, carry):
                score(zero, kh, t, fresh)
                return carry
            with jax.named_scope("att"):
                lax.fori_loop(0, 2, go, 0)

        def hop(d):
            return lax.rem(chip + CHIPS - d, CHIPS)
        block(chip, me >= 0)
        block(hop(3), me < 0)
        with jax.named_scope("att_wait"):
            @pl.when(chip == 2)
            def _():
                kv_remote(0, zero, 2).wait_recv()
            forward(0, 3)
        block(hop(2), me < 0)
        with jax.named_scope("att_wait"):
            @pl.when((chip == 1) | (chip == 3))
            def _():
                kv_remote(0, zero, 1).wait_recv()

            @pl.when(chip == 2)
            def _():
                for h in range(PIECES):
                    kv_relay(zero, h).wait_recv()
        block(hop(1), me < 0)
        with jax.named_scope("att"):
            def go2(kh, carry):
                mix(zero, kh)
                o_remote(kh).start()
                return carry
            lax.fori_loop(0, 2, go2, 0)

    def out_proj(slot):
        with jax.named_scope("o_wait"):
            for kh in range(2):
                o_remote(kh).wait()
        with jax.named_scope("wo_wait"):
            wait_w(slot)
        for t in range(5):
            col = pl.multiple_of(core * DH + t * 256, 256)
            abuf[:, pl.ds(col, 256)] = dot(obuf[...], unit(slot, t, 2048)).astype(BF16)
        a_remote().start()

    def mid_rows(j, base, keep=None):
        l = j // ROWS
        r = j % ROWS
        for t in range(0, NCHUNK, PIECE):
            rows = pl.ds(pl.multiple_of(base + t, PIECE), PIECE)
            y = rms(abuf[rows, :].astype(F32), norms[4 * l + 1])
            x = xbuf[r, rows, :]
            x1 = (x.astype(F32) + y.astype(F32)).astype(BF16)
            xbuf[r, rows, :] = x1 if keep is None else jnp.where(keep, x1, x)
            mbuf[rows, :] = rms(x1.astype(F32), norms[4 * l + 2])

    def end_rows(j, par, base, keep=None):
        l = j // ROWS
        r = j % ROWS
        for t in range(0, NCHUNK, PIECE):
            rows = pl.ds(pl.multiple_of(base + t, PIECE), PIECE)
            y = rms(dbuf[par, rows, :].astype(F32), norms[4 * l + 3])
            x = xbuf[r, rows, :]
            x2 = (x.astype(F32) + y.astype(F32)).astype(BF16)
            xbuf[r, rows, :] = x2 if keep is None else jnp.where(keep, x2, x)
            dbuf[par, rows, :] = rms(x2.astype(F32), norms[4])

    def put_out(j):
        r = j % ROWS
        return pltpu.make_async_copy(
            xbuf.at[r, pl.ds(pl.multiple_of(core * TOK, TOK), TOK), :], out_hbm.at[r], out_sem.at[r])

    pos_local().start()
    x_local(0).start()
    freq_copy().start()
    for k in range(8):
        norm_copy(k, all_norms[k]).start()
    x_local(1).start()
    x_local(2).start()
    def clear(i, carry):
        l = i // (ROWS * CHIPS)
        r = (i // CHIPS) % ROWS
        b = i % CHIPS

        @pl.when((b > chip) | ((l == 0) & (b < chip - 2)))
        def _():
            kvbuf[l, r, pl.ds(pl.multiple_of(b * CTOK, CTOK), CTOK), HKV:] = jnp.zeros((CTOK, HKV), BF16)
        return carry
    lax.fori_loop(0, 2 * ROWS * CHIPS, clear, 0)
    freq_copy().wait()
    pos_local().wait()
    start_kv(wk0, wv0, 0)
    with jax.named_scope("tables"):
        tables(core)
    barrier = pltpu.get_barrier_semaphore()
    for k in range(1, 8):
        pl.semaphore_signal(barrier, inc=1, device_id=at(lax.rem(me + k, 8)), device_id_type=MESH)
    with jax.named_scope("entry"):
        pl.semaphore_wait(barrier, 7)
    x_remote(0).start()
    for k in range(1, 8):
        pos_remote(k).start()
    for r in range(1, ROWS):
        x_remote(r).start()
    for k in range(8):
        norm_copy(k, all_norms[k]).wait()
    for k in range(8):
        norms[k] = nraw[k][...].reshape(1, DIM)

    @pl.when(core == 0)
    def _():
        pos_remote(7).wait_recv()

    @pl.when(core == 1)
    def _():
        pos_remote(1).wait_recv()
    with jax.named_scope("tables"):
        tables(1 - core)
    start_q(wq0, 1)
    start_wo(me >= 0, 2)

    def first_norm(r, carry):
        with jax.named_scope("x_wait"):
            x_local(r).wait()
            x_remote(r).wait()

        def chunk(i, carry):
            for t in range(0, NCHUNK, PIECE):
                rows = pl.ds(pl.multiple_of(i * NCHUNK + t, PIECE), PIECE)
                hpeer[r // 2, rows, pl.ds(pl.multiple_of((r % 2) * DIM, DIM), DIM)] = rms(
                    xbuf[r, rows, :].astype(F32), norms[0])
            return carry
        lax.fori_loop(0, CTOK // NCHUNK, chunk, 0)
        return carry

    start_gu(me >= 0, 0, 3)
    wait_w(0)

    def a0(r):
        return hpeer[r // 2, :, pl.ds(pl.multiple_of((r % 2) * DIM, DIM), DIM)]

    def first_kv(r, carry):
        first_norm(r, 0)
        kv_part(lambda: a0(r), 0, 0, r)
        send_kv0(r)
        return carry
    with jax.named_scope("first_kv"):
        lax.fori_loop(0, ROWS, first_kv, 0)
    start_gu(me >= 0, 1, 0)
    wait_w(1)

    def first_q(r, carry):
        q_part(lambda: a0(r), 1, r)

        @pl.when(r >= 1)
        def _():
            forward(0, r)
        return carry
    forward(0, 0)
    with jax.named_scope("first_q"):
        lax.fori_loop(0, ROWS, first_q, 0)
    start_gu(me >= 0, 2, 1)
    for k in range(1, 8):
        pos_remote(k).wait_send()

    @pl.when(core == 0)
    def _():
        for k in range(1, 7):
            pos_remote(k).wait_recv()

    @pl.when(core == 1)
    def _():
        for k in range(2, 8):
            pos_remote(k).wait_recv()
    attention()
    forward(1, 0)
    forward(1, 1)
    out_proj(2)
    forward(1, 2)
    with jax.named_scope("a_wait"):
        a_remote().wait()

    def first_mid(i, carry):
        mid_rows(0 * me, i * NCHUNK)
        return carry
    lax.fori_loop(0, CTOK // NCHUNK, first_mid, 0)
    forward(1, 3)

    def step(j, carry):
        first = j < ROWS
        first_next = j + 1 < ROWS
        more = j + 1 < STEPS
        par = j % 2
        has_qkv = (j >= 1) & (j <= ROWS)
        done = jnp.where(j >= 1, jnp.minimum(j - 1, ROWS), 0)
        extra = jnp.where(has_qkv, 2, 0)
        sb = 3 + 2 * done
        db = sb + extra + GU
        nxt = jnp.minimum(j + 1, STEPS - 1)

        def sl(p):
            return lax.rem(p, DEPTH)

        def gate_up(i, pos, beside):
            slot = sl(pos)
            with jax.named_scope("gu_wait"):
                wait_w(slot)
            base = i * 512
            prev = base - 256 if not isinstance(i, int) or i > 0 else base + 256
            hown[:, pl.ds(pl.multiple_of(prev, 256), 256)] = gated(gs[...], us[...])
            g = dot(mbuf[...], unit(slot, 0))
            u = dot(mbuf[...], unit(slot, 1))
            beside()
            hown[:, pl.ds(pl.multiple_of(base, 256), 256)] = gated(g, u)
            gs[...] = dot(mbuf[...], unit(slot, 2))
            us[...] = dot(mbuf[...], unit(slot, 3))

        @pl.when(has_qkv)
        def _():
            start_q(wq1, sl(sb + 3))

        @pl.when(jnp.logical_not(has_qkv))
        def _():
            start_gu(first, 3, sl(sb + 3))
        with jax.named_scope("gate_up0"):
            gate_up(0, sb, lambda: None)

        @pl.when(has_qkv)
        def _():
            start_gu(first, 2, sl(sb + 4))

        @pl.when(jnp.logical_not(has_qkv))
        def _():
            start_gu(first, 4, sl(sb + 4))

        @pl.when(j >= 1)
        def _():
            with jax.named_scope("d_wait"):
                d_remote(1 - par).wait()
        last = jnp.maximum(j - 1, 0)

        def ending():
            for c in range(2):
                end_rows(last, 1 - par, c * NCHUNK, j >= 1)
        with jax.named_scope("gate_up1"):
            gate_up(1, sb + 1, ending)

        @pl.when(has_qkv)
        def _():
            start_gu(first, 3, sl(sb + 5))
            wait_w(sl(sb + 2))
            with jax.named_scope("kv"):
                kv_part(lambda: dbuf[1 - par], sl(sb + 2), 1, last)
            send_kv(1, last, 3)
            start_gu(first, 4, sl(sb + 6))
            wait_w(sl(sb + 3))
            with jax.named_scope("q"):
                q_part(lambda: dbuf[1 - par], sl(sb + 3), last)

        @pl.when(j > ROWS)
        def _():
            put_out(j - 1).start()

        @pl.when(more)
        def _():
            with jax.named_scope("att_wait"):
                kv_wait(j + 1)

        def scoring(i, carry):
            pos = sb + extra + i

            @pl.when(i + 3 < GU)
            def _():
                start_gu(first, i + 3, sl(pos + 3))

            @pl.when(i + 3 >= GU)
            def _():
                start_down(first, i + 3 - GU, sl(pos + 3))
            h_remote(par, i - 2).start()
            e = i - 2
            gate_up(i, pos, lambda: score(nxt, e // CHIPS, e % CHIPS, e % CHIPS == 0))
            return carry
        with jax.named_scope("gate_up"):
            lax.fori_loop(2, GU, scoring, 0)

        hown[:, FFH - 256:FFH] = gated(gs[...], us[...])
        h_remote(par, GU - 2).start()
        h_remote(par, GU - 1).start()

        @pl.when(j == 0)
        def _():
            for h in range(PIECES):
                forward(2, h)

        def down_col(n):
            return pl.ds(pl.multiple_of(core * DH + n * 256, 256), 256)

        mine = pl.ds(pl.multiple_of(core * FFH, FFH), FFH)
        other = pl.ds(pl.multiple_of((1 - core) * FFH, FFH), FFH)
        def pair(lhs, sa, sb_, rows, out_a, out_b):
            y = dot(lhs, jnp.concatenate([ring[sa, rows, :], ring[sb_, rows, :]], axis=1))
            out_a[...] = y[:, :256]
            out_b[...] = y[:, 256:]

        def half_down(n, pos, k):
            row = pl.multiple_of((core + k - 2 * core * k) * FFH, FFH)

            def go(wd):
                pltpu.make_async_copy(
                    wd.at[pl.ds(row, FFH), pl.ds(pl.multiple_of(core * DH + n * 256, 256), 256)],
                    ring.at[sl(pos), pl.ds(row, FFH), :], half_sem.at[k, n - 3]).start()
            by_layer(first, lambda: go(wd0), lambda: go(wd1))

        def half_wait(n, pos, k):
            row = pl.multiple_of((core + k - 2 * core * k) * FFH, FFH)
            pltpu.make_async_copy(
                wd0.at[pl.ds(row, FFH), pl.ds(0, 256)], ring.at[sl(pos), pl.ds(row, FFH), :],
                half_sem.at[k, n - 3]).wait()

        p3 = db + 3 + jnp.where(more, 1, 0)
        p4 = p3 + 1
        with jax.named_scope("down_a"):
            @pl.when(more)
            def _():
                start_wo(first_next, sl(db + 3))

            @pl.when(jnp.logical_not(more))
            def _():
                half_down(3, p3, 0)
                half_down(3, p3, 1)
            wait_w(sl(db))
            wait_w(sl(db + 1))
            pair(hown[...], sl(db), sl(db + 1), mine, gs, us)
            mix(nxt, 0)

            @pl.when(more)
            def _():
                o_remote(0).start()
                half_down(3, p3, 0)
            half_down(4, p4, 0)
            with jax.named_scope("h_wait"):
                h_all(par).wait()
            pair(hpeer[par], sl(db), sl(db + 1), other, gb, ub)
            mix(nxt, 1)
            dbuf[par, :, down_col(0)] = (gs[...] + gb[...]).astype(BF16)
            dbuf[par, :, down_col(1)] = (us[...] + ub[...]).astype(BF16)

            @pl.when(more)
            def _():
                o_remote(1).start()
                half_down(3, p3, 1)
            half_down(4, p4, 1)

        with jax.named_scope("down2"):
            wait_w(sl(db + 2))
            gs[...] = dot(hown[...], ring[sl(db + 2), mine, :])
            us[...] = dot(hpeer[par], ring[sl(db + 2), other, :])
            dbuf[par, :, down_col(2)] = (gs[...] + us[...]).astype(BF16)

        @pl.when(more)
        def _():
            start_gu(first_next, 0, sl(db + 6))
            with jax.named_scope("proj"):
                out_proj(sl(db + 3))
            start_gu(first_next, 1, sl(db + 7))
        s3 = sl(p3)
        s4 = sl(p4)
        with jax.named_scope("down3"):
            with jax.named_scope("dn_wait"):
                half_wait(3, p3, 0)
                half_wait(4, p4, 0)
            pair(hown[...], s3, s4, mine, gs, us)

        @pl.when(more)
        def _():
            with jax.named_scope("a_wait"):
                a_remote().wait()

        with jax.named_scope("down4"):
            with jax.named_scope("dn_wait"):
                half_wait(3, p3, 1)
                half_wait(4, p4, 1)
            pair(hpeer[par], s3, s4, other, gb, ub)
            for c in range(2):
                mid_rows(nxt, c * NCHUNK, more)
            dbuf[par, :, down_col(3)] = (gs[...] + gb[...]).astype(BF16)
            dbuf[par, :, down_col(4)] = (us[...] + ub[...]).astype(BF16)

        @pl.when(more)
        def _():
            @pl.when(j + 1 <= ROWS)
            def _():
                start_kv(wk1, wv1, sl(db + 8))

            @pl.when(j + 1 > ROWS)
            def _():
                start_gu(first_next, 2, sl(db + 8))
        d_remote(par).start()
        return carry

    lax.fori_loop(0, STEPS, step, 0)

    d_remote((STEPS - 1) % 2).wait()

    def final(i, carry):
        end_rows(STEPS - 1 + 0 * me, (STEPS - 1) % 2, core * TOK + i * NCHUNK)
        return carry
    lax.fori_loop(0, TOK // NCHUNK, final, 0)
    put_out(STEPS - 1).start()
    for r in range(ROWS):
        put_out(r).wait()
    for r in range(ROWS):
        for d in range(1, CHIPS):
            @pl.when(chip + d < CHIPS)
            def _(r=r, d=d):
                kv_remote(1, r, d).wait_send()

        @pl.when(chip == 0)
        def _(r=r):
            kv_remote(0, r, 2).wait_send()

        @pl.when((chip == 0) | (chip == 2))
        def _(r=r):
            kv_remote(0, r, 1).wait_send()

        @pl.when(chip == 1)
        def _(r=r):
            for h in range(PIECES):
                kv_second(r, h).wait_send()

        @pl.when(chip == 3)
        def _(r=r):
            for h in range(PIECES):
                kv_relay(r, h).wait_send()


def solution(mesh):
    def device_step(hidden, positions, *weights):
        local_w = weights[:11]
        global_w = weights[11:]
        half_dim = HEAD_DIM // 2
        inv_freq = (THETA ** (-(np.arange(half_dim, dtype=np.float64) * 2.0 / HEAD_DIM))).astype(np.float32)
        freq = jnp.asarray(inv_freq.reshape(1, half_dim))
        norms = local_w[7:11] + global_w[7:11]
        hbm = pl.BlockSpec(memory_space=pltpu.HBM)
        dma = pltpu.SemaphoreType.DMA
        flops = 2 * ROWS * TOK * 2 * (DIM * 4096 + 2048 * DIM + 3 * DIM * FF)
        return pl.pallas_call(
            kernel,
            out_shape=jax.ShapeDtypeStruct(hidden.shape, hidden.dtype),
            in_specs=[hbm] * 25,
            out_specs=hbm,
            scratch_shapes=[
                pltpu.VMEM((DEPTH, FF, 256), BF16),
                pltpu.VMEM((2, ROWS, KEYS, 2 * HKV), BF16),
                pltpu.VMEM((ROWS, CTOK, DIM), BF16),
                pltpu.VMEM((CTOK, DIM), BF16),
                pltpu.VMEM((CTOK, FFH), BF16),
                pltpu.VMEM((2, CTOK, FFH), BF16),
                pltpu.VMEM((ROWS, 4, CTOK, HEAD_DIM), BF16),
                pltpu.VMEM((CTOK, 2 * HQ), BF16),
                pltpu.VMEM((CTOK, DIM), BF16),
                pltpu.VMEM((2, CTOK, DIM), BF16),
                pltpu.VMEM((2, ROWS, TOK, 128), F32),
                pltpu.VMEM((2, ROWS, TOK, 128), F32),
                pltpu.VMEM((2, ROWS, TOK, 128), jnp.int32),
                pltpu.VMEM((8, ROWS, 128), jnp.int32),
                pltpu.VMEM((1, 128), F32),
                pltpu.VMEM((8, 1, DIM), F32),
                *[pltpu.VMEM((DIM,), F32)] * 8,
                pltpu.VMEM((4, CTOK, KEYS), F32),
                pltpu.VMEM((4, CTOK, 128), F32),
                *[pltpu.VMEM((CTOK, 256), F32)] * 4,
                dma((9,)), dma((DEPTH,)), dma((2, 2)), dma((ROWS,)), dma((ROWS,)), dma((ROWS,)),
                dma((8,)), dma((8,)),
                dma((2, ROWS, CHIPS)), dma((2, ROWS, CHIPS)), dma((ROWS, PIECES)), dma((ROWS, PIECES)),
                dma((2,)), dma((2,)), dma, dma,
                dma((2,)), dma((2,)), dma((2,)), dma((2,)), dma((ROWS,)),
            ],
            compiler_params=pltpu.CompilerParams(
                collective_id=0, has_side_effects=True, vmem_limit_bytes=67043328),
            cost_estimate=pl.CostEstimate(flops=flops, bytes_accessed=600000000, transcendentals=0),
            name="layers",
        )(hidden, positions, freq, *norms, *local_w[:7], *global_w[:7])

    specs_in = tuple([P("dp", "cp"), P("dp", "cp")] + [P()] * 22)
    return jax.shard_map(device_step, mesh=mesh, in_specs=specs_in, out_specs=P("dp", "cp"), check_vma=False)
```

```python
import functools
import math

import jax
import jax.numpy as jnp
import numpy as np
from jax import lax
from jax.experimental import pallas as pl
from jax.experimental.pallas import tpu as pltpu
from jax.sharding import PartitionSpec as P

HEAD_DIM = 256
WINDOW = 512
EPSILON = 1e-6
THETA = 10000.0
SOFT_CAP = 50.0
EXP2_CAP = SOFT_CAP * math.log2(math.e)

MESH = pl.DeviceIdType.MESH
F32 = jnp.float32
BF16 = jnp.bfloat16

ROWS = 3
TOK = 128
CTOK = 256
DIM = 2560
HQ = 1024
HKV = 512
FF = 10240
FFH = FF // 2
DH = DIM // 2
CHIPS = 4
STEPS = 2 * ROWS
DEPTH = 4
GU = FFH // 512
SCORES = 8
NCHUNK = 128
PIECE = 16
PIECES = 8
PTOK = CTOK // PIECES
KEYS = CHIPS * CTOK


def dot(a, b):
    return jnp.dot(a, b, preferred_element_type=F32)


def rms(u, w):
    mean_sq = jnp.mean(u * u, axis=-1, keepdims=True)
    return (u * lax.rsqrt(mean_sq + EPSILON) * (1.0 + w)).astype(BF16)


def gated(g, u):
    g = g.astype(BF16).astype(F32)
    u = u.astype(BF16).astype(F32)
    return (jax.nn.gelu(g, approximate=True) * u).astype(BF16)


def kernel(x_hbm, pos_in, freq_in, n0, n1, n2, n3, n4, n5, n6, n7,
           wq0, wk0, wv0, wo0, wg0, wu0, wd0, wq1, wk1, wv1, wo1, wg1, wu1, wd1,
           out_hbm,
           ring, kvbuf, xbuf, mbuf, hown, hpeer, qbuf, obuf, abuf, dbuf, cosb, sinb, tposb, posbuf, freq, norms, r0, r1, r2, r3, r4, r5, r6, r7, ebuf, sbuf, gs, us, gb, ub,
           n_sem, ring_sem, half_sem, xl_sem, xs_sem, xr_sem, ps_sem, pr_sem, kvs_sem, kvr_sem, ks_sem, kr_sem,
           os_sem, or_sem, as_sem, ar_sem, hs_sem, hr_sem, dss_sem, dr_sem, out_sem):
    me = lax.axis_index("cp")
    chip = me // 2
    core = me % 2
    peer = me + 1 - 2 * core

    def at(dev):
        return {"cp": dev}

    def start_cols(w, rows, col, slot, row0):
        pltpu.make_async_copy(
            w.at[pl.ds(0, rows), pl.ds(pl.multiple_of(col, 256), 256)],
            ring.at[slot, pl.ds(row0, rows), :], ring_sem.at[slot]).start()

    def by_layer(first, f0, f1):
        @pl.when(first)
        def _():
            f0()

        @pl.when(jnp.logical_not(first))
        def _():
            f1()

    def start_gu(first, i, slot):
        def go(wg, wu):
            col = core * FFH + i * 512
            for t in range(2):
                start_cols(wg, DIM, col + 256 * t, slot, 2 * t * DIM)
                start_cols(wu, DIM, col + 256 * t, slot, (2 * t + 1) * DIM)
        by_layer(first, lambda: go(wg0, wu0), lambda: go(wg1, wu1))

    def start_down(first, n, slot):
        def go(wd):
            start_cols(wd, FF, core * DH + n * 256, slot, 0)
        by_layer(first, lambda: go(wd0), lambda: go(wd1))

    def start_wo(first, slot):
        def go(wo):
            for t in range(5):
                start_cols(wo, 2048, core * DH + t * 256, slot, t * 2048)
        by_layer(first, lambda: go(wo0), lambda: go(wo1))

    def start_kv(wk, wv, slot):
        for t in range(2):
            start_cols(wk, DIM, core * HKV + t * 256, slot, t * DIM)
            start_cols(wv, DIM, core * HKV + t * 256, slot, (2 + t) * DIM)

    def start_q(wq, slot):
        for t in range(4):
            start_cols(wq, DIM, core * HQ + t * 256, slot, t * DIM)

    def wait_w(slot):
        pltpu.make_async_copy(wd0.at[:, pl.ds(0, 256)], ring.at[slot], ring_sem.at[slot]).wait()

    def unit(slot, t, rows=DIM):
        return ring[slot, pl.ds(t * rows, rows), :]

    def x_local(r):
        return pltpu.make_async_copy(
            x_hbm.at[r], xbuf.at[r, pl.ds(pl.multiple_of(core * TOK, TOK), TOK), :], xl_sem.at[r])

    def x_remote(r):
        return pltpu.make_async_remote_copy(
            x_hbm.at[r], xbuf.at[r, pl.ds(pl.multiple_of(core * TOK, TOK), TOK), :],
            xs_sem.at[r], xr_sem.at[r], device_id=at(peer), device_id_type=MESH)

    def norm_copy(k, src):
        return pltpu.make_async_copy(src, nraw[k], n_sem.at[k])

    all_norms = (n0, n1, n2, n3, n4, n5, n6, n7)
    nraw = (r0, r1, r2, r3, r4, r5, r6, r7)

    def freq_copy():
        return pltpu.make_async_copy(freq_in, freq, n_sem.at[8])

    def tables(c):
        rows = posbuf[2 * chip + c].astype(F32)
        cols = jnp.transpose(jnp.concatenate([rows, jnp.zeros((TOK - ROWS, TOK), F32)], axis=0))
        for r in range(ROWS):
            col = jnp.broadcast_to(cols[:, r:r + 1], (TOK, 128))
            tposb[c, r] = col.astype(jnp.int32)
            angle = col * freq[...]
            cosb[c, r] = jnp.cos(angle)
            sinb[c, r] = jnp.sin(angle)

    def pos_local():
        return pltpu.make_async_copy(pos_in, posbuf.at[me], ps_sem.at[0])

    def pos_remote(k):
        return pltpu.make_async_remote_copy(
            pos_in, posbuf.at[me], ps_sem.at[k], pr_sem.at[k],
            device_id=at(lax.rem(me + k, 8)), device_id_type=MESH)

    def kv_own(l, r):
        return kvbuf.at[l, r, pl.ds(pl.multiple_of(chip * CTOK, CTOK), CTOK), :]

    def kv_remote(l, r, d):
        return pltpu.make_async_remote_copy(
            kv_own(l, r), kv_own(l, r), kvs_sem.at[l, r, d], kvr_sem.at[l, r, d],
            device_id=at(lax.rem(me + 2 * d, 8)), device_id_type=MESH)

    def kv_piece(r, h):
        return kvbuf.at[0, r, pl.ds(pl.multiple_of(CTOK + h * PTOK, PTOK), PTOK), :]

    def kv_second(r, h):
        return pltpu.make_async_remote_copy(
            kv_piece(r, h), kv_piece(r, h), ks_sem.at[r, h], kr_sem.at[r, h],
            device_id=at(6 + core), device_id_type=MESH)

    def kv_relay(r, h):
        return pltpu.make_async_remote_copy(
            kv_piece(r, h), kv_piece(r, h), ks_sem.at[r, h], kr_sem.at[r, h],
            device_id=at(4 + core), device_id_type=MESH)

    def forward(r, h):
        @pl.when(chip == 3)
        def _():
            kv_second(r, h).wait_recv()
            kv_relay(r, h).start()

    def send_kv0(r):
        @pl.when(chip == 0)
        def _():
            kv_remote(0, r, 2).start()
            kv_remote(0, r, 1).start()

        @pl.when(chip == 1)
        def _():
            for h in range(PIECES):
                kv_second(r, h).start()

        @pl.when(chip == 2)
        def _():
            kv_remote(0, r, 1).start()

    def half(buf, width):
        return buf.at[:, pl.ds(pl.multiple_of(core * width, 256), width)]

    def o_remote(kh):
        cols = obuf.at[:, pl.ds(pl.multiple_of(core * HQ + kh * 512, 512), 512)]
        return pltpu.make_async_remote_copy(
            cols, cols, os_sem.at[kh], or_sem.at[kh], device_id=at(peer), device_id_type=MESH)

    def a_remote():
        return pltpu.make_async_remote_copy(
            half(abuf, DH), half(abuf, DH), as_sem, ar_sem, device_id=at(peer), device_id_type=MESH)

    def d_remote(par, k):
        width = 768 - 256 * k
        cols = dbuf.at[par, :, pl.ds(pl.multiple_of(core * DH + k * 768, 256), width)]
        return pltpu.make_async_remote_copy(
            cols, cols, dss_sem.at[par, k], dr_sem.at[par, k], device_id=at(peer), device_id_type=MESH)

    def h_remote(par, i):
        cols = pl.ds(pl.multiple_of(i * 512, 512), 512)
        return pltpu.make_async_remote_copy(
            hown.at[:, cols], hpeer.at[par, :, cols], hs_sem.at[par], hr_sem.at[par],
            device_id=at(peer), device_id_type=MESH)

    def h_all(par):
        return pltpu.make_async_remote_copy(
            hown, hpeer.at[par], hs_sem.at[par], hr_sem.at[par], device_id=at(peer), device_id_type=MESH)

    def rope(y, r, t, dst):
        y = y.astype(BF16).astype(F32)
        for c in range(2):
            f = y[c * TOK:(c + 1) * TOK, :128]
            s = y[c * TOK:(c + 1) * TOK, 128:]
            cos = cosb[c, r]
            sin = sinb[c, r]
            dst(c, (f * cos - s * sin) * t, (s * cos + f * sin) * t)

    def kv_part(src, slot, l, r):
        for t in range(2):
            y = dot(src(), unit(slot, t))

            def put(c, a, b, t=t):
                rows = pl.ds(pl.multiple_of(chip * CTOK + c * TOK, TOK), TOK)
                kvbuf[l, r, rows, t * 256:t * 256 + 128] = a.astype(BF16)
                kvbuf[l, r, rows, t * 256 + 128:t * 256 + 256] = b.astype(BF16)
            rope(y, r, 1.0, put)
            kvbuf[l, r, pl.ds(pl.multiple_of(chip * CTOK, CTOK), CTOK), HKV + t * 256:HKV + t * 256 + 256] = dot(src(), unit(slot, 2 + t)).astype(BF16)

    def q_part(src, slot, r):
        for t in range(4):
            y = dot(src(), unit(slot, t))

            def put(c, a, b, t=t):
                rows = pl.ds(c * TOK, TOK)
                qbuf[r, t, rows, 0:128] = a.astype(BF16)
                qbuf[r, t, rows, 128:256] = b.astype(BF16)
            rope(y, r, HEAD_DIM ** -0.5, put)

    def send_kv(l, r, far):
        for d in range(1, far + 1):
            @pl.when(chip + d < CHIPS)
            def _(d=d):
                kv_remote(l, r, d).start()

    def kv_wait(j):
        l = j // ROWS
        r = j % ROWS
        for d in range(1, CHIPS):
            @pl.when((chip - d >= 0) & (l == 1))
            def _(d=d):
                kv_remote(1, r, d).wait_recv()

        @pl.when(l == 0)
        def _():
            @pl.when((chip == 1) | (chip == 3))
            def _():
                kv_remote(0, r, 1).wait_recv()

            @pl.when(chip == 2)
            def _():
                kv_remote(0, r, 2).wait_recv()
                for h in range(PIECES):
                    kv_relay(r, h).wait_recv()

    def score(j, kh, t, fresh):
        l = j // ROWS
        r = j % ROWS
        reach = WINDOW + l * 1000000
        k = kvbuf[l, r, pl.ds(pl.multiple_of(t * CTOK, CTOK), CTOK), pl.ds(pl.multiple_of(kh * 256, 256), 256)]
        masks = {}
        for c in range(2):
            for kc in range(2):
                off = tposb[c, r] - posbuf[2 * t + kc, pl.ds(r, 1), :]
                masks[c, kc] = (off >= 0) & (off < reach)
        for hh in range(2):
            q = qbuf[r, 2 * kh + hh]
            s = lax.dot_general(q, k, (((1,), (1,)), ((), ())), preferred_element_type=F32)
            e = jnp.exp2(EXP2_CAP * jnp.tanh(s * (1.0 / SOFT_CAP)))
            for c in range(2):
                rows = slice(c * TOK, (c + 1) * TOK)
                tot = jnp.where(fresh, 0.0, sbuf[2 * kh + hh, rows, :])
                for kc in range(2):
                    piece = jnp.where(masks[c, kc], e[rows, kc * 128:(kc + 1) * 128], 0.0)
                    ebuf[2 * kh + hh, rows, pl.ds(pl.multiple_of(t * CTOK + kc * 128, 128), 128)] = piece
                    tot = tot + piece
                sbuf[2 * kh + hh, rows, :] = tot

    def mix(j, kh):
        l = j // ROWS
        r = j % ROWS
        v = kvbuf[l, r, :, pl.ds(pl.multiple_of(HKV + kh * 256, 256), 256)]
        for hh in range(2):
            inv = 1.0 / jnp.sum(sbuf[2 * kh + hh], axis=-1, keepdims=True)
            p = (ebuf[2 * kh + hh] * inv).astype(BF16)
            col = pl.multiple_of(core * HQ + (2 * kh + hh) * 256, 256)
            obuf[:, pl.ds(col, 256)] = dot(p, v).astype(BF16)

    def attention():
        zero = 0 * me

        def block(t, fresh):
            def go(kh, carry):
                score(zero, kh, t, fresh)
                return carry
            with jax.named_scope("att"):
                lax.fori_loop(0, 2, go, 0)

        def hop(d):
            return lax.rem(chip + CHIPS - d, CHIPS)
        block(chip, me >= 0)
        block(hop(3), me < 0)
        with jax.named_scope("att_wait"):
            @pl.when(chip == 2)
            def _():
                kv_remote(0, zero, 2).wait_recv()
            forward(0, 7)
        block(hop(2), me < 0)
        with jax.named_scope("att_wait"):
            @pl.when((chip == 1) | (chip == 3))
            def _():
                kv_remote(0, zero, 1).wait_recv()

            @pl.when(chip == 2)
            def _():
                for h in range(PIECES):
                    kv_relay(zero, h).wait_recv()
        block(hop(1), me < 0)
        with jax.named_scope("att"):
            def go2(kh, carry):
                mix(zero, kh)
                o_remote(kh).start()
                return carry
            lax.fori_loop(0, 2, go2, 0)

    def out_proj(slot):
        with jax.named_scope("o_wait"):
            for kh in range(2):
                o_remote(kh).wait()
        with jax.named_scope("wo_wait"):
            wait_w(slot)
        for t in range(5):
            col = pl.multiple_of(core * DH + t * 256, 256)
            abuf[:, pl.ds(col, 256)] = dot(obuf[...], unit(slot, t, 2048)).astype(BF16)
        a_remote().start()

    def mid_rows(j, base, keep=None):
        l = j // ROWS
        r = j % ROWS
        for t in range(0, NCHUNK, PIECE):
            rows = pl.ds(pl.multiple_of(base + t, PIECE), PIECE)
            y = rms(abuf[rows, :].astype(F32), norms[4 * l + 1])
            x = xbuf[r, rows, :]
            x1 = (x.astype(F32) + y.astype(F32)).astype(BF16)
            xbuf[r, rows, :] = x1 if keep is None else jnp.where(keep, x1, x)
            mbuf[rows, :] = rms(x1.astype(F32), norms[4 * l + 2])

    def end_rows(j, par, base, keep=None):
        l = j // ROWS
        r = j % ROWS
        for t in range(0, NCHUNK, PIECE):
            rows = pl.ds(pl.multiple_of(base + t, PIECE), PIECE)
            y = rms(dbuf[par, rows, :].astype(F32), norms[4 * l + 3])
            x = xbuf[r, rows, :]
            x2 = (x.astype(F32) + y.astype(F32)).astype(BF16)
            xbuf[r, rows, :] = x2 if keep is None else jnp.where(keep, x2, x)
            dbuf[par, rows, :] = rms(x2.astype(F32), norms[4])

    def put_out(j):
        r = j % ROWS
        return pltpu.make_async_copy(
            xbuf.at[r, pl.ds(pl.multiple_of(core * TOK, TOK), TOK), :], out_hbm.at[r], out_sem.at[r])

    pos_local().start()
    x_local(0).start()
    freq_copy().start()
    for k in range(8):
        norm_copy(k, all_norms[k]).start()
    x_local(1).start()
    x_local(2).start()
    def clear(i, carry):
        l = i // (ROWS * CHIPS)
        r = (i // CHIPS) % ROWS
        b = i % CHIPS

        @pl.when((b > chip) | ((l == 0) & (b < chip - 2)))
        def _():
            kvbuf[l, r, pl.ds(pl.multiple_of(b * CTOK, CTOK), CTOK), HKV:] = jnp.zeros((CTOK, HKV), BF16)
        return carry
    lax.fori_loop(0, 2 * ROWS * CHIPS, clear, 0)
    freq_copy().wait()
    pos_local().wait()
    start_kv(wk0, wv0, 0)
    with jax.named_scope("tables"):
        tables(core)
    barrier = pltpu.get_barrier_semaphore()
    for k in range(1, 8):
        pl.semaphore_signal(barrier, inc=1, device_id=at(lax.rem(me + k, 8)), device_id_type=MESH)
    with jax.named_scope("entry"):
        pl.semaphore_wait(barrier, 7)
    x_remote(0).start()
    for k in range(1, 8):
        pos_remote(k).start()
    for r in range(1, ROWS):
        x_remote(r).start()
    for k in range(8):
        norm_copy(k, all_norms[k]).wait()
    for k in range(8):
        norms[k] = nraw[k][...].reshape(1, DIM)

    @pl.when(core == 0)
    def _():
        pos_remote(7).wait_recv()

    @pl.when(core == 1)
    def _():
        pos_remote(1).wait_recv()
    with jax.named_scope("tables"):
        tables(1 - core)
    start_q(wq0, 1)
    start_wo(me >= 0, 2)

    def first_norm(r, carry):
        with jax.named_scope("x_wait"):
            x_local(r).wait()
            x_remote(r).wait()

        def chunk(i, carry):
            for t in range(0, NCHUNK, PIECE):
                rows = pl.ds(pl.multiple_of(i * NCHUNK + t, PIECE), PIECE)
                hpeer[r // 2, rows, pl.ds(pl.multiple_of((r % 2) * DIM, DIM), DIM)] = rms(
                    xbuf[r, rows, :].astype(F32), norms[0])
            return carry
        lax.fori_loop(0, CTOK // NCHUNK, chunk, 0)
        return carry

    start_gu(me >= 0, 0, 3)
    wait_w(0)

    def a0(r):
        return hpeer[r // 2, :, pl.ds(pl.multiple_of((r % 2) * DIM, DIM), DIM)]

    def first_kv(r, carry):
        first_norm(r, 0)
        kv_part(lambda: a0(r), 0, 0, r)
        send_kv0(r)
        return carry
    with jax.named_scope("first_kv"):
        lax.fori_loop(0, ROWS, first_kv, 0)
    start_gu(me >= 0, 1, 0)
    wait_w(1)

    def first_q(r, carry):
        q_part(lambda: a0(r), 1, r)

        forward(0, 2 * r + 2)

        @pl.when(r <= 1)
        def _():
            forward(0, 2 * r + 3)
        return carry
    forward(0, 0)
    forward(0, 1)
    with jax.named_scope("first_q"):
        lax.fori_loop(0, ROWS, first_q, 0)
    start_gu(me >= 0, 2, 1)
    for k in range(1, 8):
        pos_remote(k).wait_send()

    @pl.when(core == 0)
    def _():
        for k in range(1, 7):
            pos_remote(k).wait_recv()

    @pl.when(core == 1)
    def _():
        for k in range(2, 8):
            pos_remote(k).wait_recv()
    attention()
    for h in range(4):
        forward(1, h)
    out_proj(2)
    forward(1, 4)
    forward(1, 5)
    with jax.named_scope("a_wait"):
        a_remote().wait()

    def first_mid(i, carry):
        mid_rows(0 * me, i * NCHUNK)
        return carry
    lax.fori_loop(0, CTOK // NCHUNK, first_mid, 0)
    forward(1, 6)
    forward(1, 7)

    def step(j, carry):
        first = j < ROWS
        first_next = j + 1 < ROWS
        more = j + 1 < STEPS
        par = j % 2
        has_qkv = (j >= 1) & (j <= ROWS)
        done = jnp.where(j >= 1, jnp.minimum(j - 1, ROWS), 0)
        extra = jnp.where(has_qkv, 2, 0)
        sb = 3 + 2 * done
        db = sb + extra + GU
        nxt = jnp.minimum(j + 1, STEPS - 1)

        def sl(p):
            return lax.rem(p, DEPTH)

        def gate_up(i, pos, beside):
            slot = sl(pos)
            with jax.named_scope("gu_wait"):
                wait_w(slot)
            base = i * 512
            prev = base - 256 if not isinstance(i, int) or i > 0 else base + 256
            hown[:, pl.ds(pl.multiple_of(prev, 256), 256)] = gated(gs[...], us[...])
            g = dot(mbuf[...], unit(slot, 0))
            u = dot(mbuf[...], unit(slot, 1))
            beside()
            hown[:, pl.ds(pl.multiple_of(base, 256), 256)] = gated(g, u)
            gs[...] = dot(mbuf[...], unit(slot, 2))
            us[...] = dot(mbuf[...], unit(slot, 3))

        @pl.when(has_qkv)
        def _():
            start_q(wq1, sl(sb + 3))

        @pl.when(jnp.logical_not(has_qkv))
        def _():
            start_gu(first, 3, sl(sb + 3))
        with jax.named_scope("gate_up0"):
            gate_up(0, sb, lambda: None)

        @pl.when(has_qkv)
        def _():
            start_gu(first, 2, sl(sb + 4))

        @pl.when(jnp.logical_not(has_qkv))
        def _():
            start_gu(first, 4, sl(sb + 4))

        @pl.when(j >= 1)
        def _():
            with jax.named_scope("d_wait"):
                for k in range(2):
                    d_remote(1 - par, k).wait()
        last = jnp.maximum(j - 1, 0)

        def ending():
            for c in range(2):
                end_rows(last, 1 - par, c * NCHUNK, j >= 1)
        with jax.named_scope("gate_up1"):
            gate_up(1, sb + 1, ending)

        @pl.when(has_qkv)
        def _():
            start_gu(first, 3, sl(sb + 5))
            wait_w(sl(sb + 2))
            with jax.named_scope("kv"):
                kv_part(lambda: dbuf[1 - par], sl(sb + 2), 1, last)
            send_kv(1, last, 3)
            start_gu(first, 4, sl(sb + 6))
            wait_w(sl(sb + 3))
            with jax.named_scope("q"):
                q_part(lambda: dbuf[1 - par], sl(sb + 3), last)

        @pl.when(j > ROWS)
        def _():
            put_out(j - 1).start()

        @pl.when(more)
        def _():
            with jax.named_scope("att_wait"):
                kv_wait(j + 1)

        def scoring(i, carry):
            pos = sb + extra + i

            @pl.when(i + 3 < GU)
            def _():
                start_gu(first, i + 3, sl(pos + 3))

            @pl.when(i + 3 >= GU)
            def _():
                start_down(first, i + 3 - GU, sl(pos + 3))
            h_remote(par, i - 2).start()
            e = i - 2
            gate_up(i, pos, lambda: score(nxt, e // CHIPS, e % CHIPS, e % CHIPS == 0))
            return carry
        with jax.named_scope("gate_up"):
            lax.fori_loop(2, GU, scoring, 0)

        hown[:, FFH - 256:FFH] = gated(gs[...], us[...])
        h_remote(par, GU - 2).start()
        h_remote(par, GU - 1).start()

        @pl.when(j == 0)
        def _():
            for h in range(PIECES):
                forward(2, h)

        def down_col(n):
            return pl.ds(pl.multiple_of(core * DH + n * 256, 256), 256)

        mine = pl.ds(pl.multiple_of(core * FFH, FFH), FFH)
        other = pl.ds(pl.multiple_of((1 - core) * FFH, FFH), FFH)
        def pair(lhs, sa, sb_, rows, out_a, out_b):
            y = dot(lhs, jnp.concatenate([ring[sa, rows, :], ring[sb_, rows, :]], axis=1))
            out_a[...] = y[:, :256]
            out_b[...] = y[:, 256:]

        def half_down(n, pos, k):
            row = pl.multiple_of((core + k - 2 * core * k) * FFH, FFH)

            def go(wd):
                pltpu.make_async_copy(
                    wd.at[pl.ds(row, FFH), pl.ds(pl.multiple_of(core * DH + n * 256, 256), 256)],
                    ring.at[sl(pos), pl.ds(row, FFH), :], half_sem.at[k, n - 3]).start()
            by_layer(first, lambda: go(wd0), lambda: go(wd1))

        def half_wait(n, pos, k):
            row = pl.multiple_of((core + k - 2 * core * k) * FFH, FFH)
            pltpu.make_async_copy(
                wd0.at[pl.ds(row, FFH), pl.ds(0, 256)], ring.at[sl(pos), pl.ds(row, FFH), :],
                half_sem.at[k, n - 3]).wait()

        p3 = db + 3 + jnp.where(more, 1, 0)
        p4 = p3 + 1
        with jax.named_scope("down_a"):
            @pl.when(more)
            def _():
                start_wo(first_next, sl(db + 3))

            @pl.when(jnp.logical_not(more))
            def _():
                half_down(3, p3, 0)
                half_down(3, p3, 1)
            wait_w(sl(db))
            wait_w(sl(db + 1))
            pair(hown[...], sl(db), sl(db + 1), mine, gs, us)
            mix(nxt, 0)

            @pl.when(more)
            def _():
                o_remote(0).start()
                half_down(3, p3, 0)
            half_down(4, p4, 0)
            with jax.named_scope("h_wait"):
                h_all(par).wait()
            pair(hpeer[par], sl(db), sl(db + 1), other, gb, ub)
            mix(nxt, 1)
            dbuf[par, :, down_col(0)] = (gs[...] + gb[...]).astype(BF16)
            dbuf[par, :, down_col(1)] = (us[...] + ub[...]).astype(BF16)

            @pl.when(more)
            def _():
                o_remote(1).start()
                half_down(3, p3, 1)
            half_down(4, p4, 1)

        with jax.named_scope("down2"):
            wait_w(sl(db + 2))
            gs[...] = dot(hown[...], ring[sl(db + 2), mine, :])
            us[...] = dot(hpeer[par], ring[sl(db + 2), other, :])
            dbuf[par, :, down_col(2)] = (gs[...] + us[...]).astype(BF16)
            d_remote(par, 0).start()

        @pl.when(more)
        def _():
            start_gu(first_next, 0, sl(db + 6))
            with jax.named_scope("proj"):
                out_proj(sl(db + 3))
            start_gu(first_next, 1, sl(db + 7))
        s3 = sl(p3)
        s4 = sl(p4)
        with jax.named_scope("down3"):
            with jax.named_scope("dn_wait"):
                half_wait(3, p3, 0)
                half_wait(4, p4, 0)
            pair(hown[...], s3, s4, mine, gs, us)

        @pl.when(more)
        def _():
            with jax.named_scope("a_wait"):
                a_remote().wait()

        with jax.named_scope("down4"):
            with jax.named_scope("dn_wait"):
                half_wait(3, p3, 1)
                half_wait(4, p4, 1)
            pair(hpeer[par], s3, s4, other, gb, ub)
            for c in range(2):
                mid_rows(nxt, c * NCHUNK, more)
            dbuf[par, :, down_col(3)] = (gs[...] + gb[...]).astype(BF16)
            dbuf[par, :, down_col(4)] = (us[...] + ub[...]).astype(BF16)

        @pl.when(more)
        def _():
            @pl.when(j + 1 <= ROWS)
            def _():
                start_kv(wk1, wv1, sl(db + 8))

            @pl.when(j + 1 > ROWS)
            def _():
                start_gu(first_next, 2, sl(db + 8))
        d_remote(par, 1).start()
        return carry

    lax.fori_loop(0, STEPS, step, 0)

    for k in range(2):
        d_remote((STEPS - 1) % 2, k).wait()

    def final(i, carry):
        end_rows(STEPS - 1 + 0 * me, (STEPS - 1) % 2, core * TOK + i * NCHUNK)
        return carry
    lax.fori_loop(0, TOK // NCHUNK, final, 0)
    put_out(STEPS - 1).start()
    for r in range(ROWS):
        put_out(r).wait()
    for r in range(ROWS):
        for d in range(1, CHIPS):
            @pl.when(chip + d < CHIPS)
            def _(r=r, d=d):
                kv_remote(1, r, d).wait_send()

        @pl.when(chip == 0)
        def _(r=r):
            kv_remote(0, r, 2).wait_send()

        @pl.when((chip == 0) | (chip == 2))
        def _(r=r):
            kv_remote(0, r, 1).wait_send()

        @pl.when(chip == 1)
        def _(r=r):
            for h in range(PIECES):
                kv_second(r, h).wait_send()

        @pl.when(chip == 3)
        def _(r=r):
            for h in range(PIECES):
                kv_relay(r, h).wait_send()


def solution(mesh):
    def device_step(hidden, positions, *weights):
        local_w = weights[:11]
        global_w = weights[11:]
        half_dim = HEAD_DIM // 2
        inv_freq = (THETA ** (-(np.arange(half_dim, dtype=np.float64) * 2.0 / HEAD_DIM))).astype(np.float32)
        freq = jnp.asarray(inv_freq.reshape(1, half_dim))
        norms = local_w[7:11] + global_w[7:11]
        hbm = pl.BlockSpec(memory_space=pltpu.HBM)
        dma = pltpu.SemaphoreType.DMA
        flops = 2 * ROWS * TOK * 2 * (DIM * 4096 + 2048 * DIM + 3 * DIM * FF)
        return pl.pallas_call(
            kernel,
            out_shape=jax.ShapeDtypeStruct(hidden.shape, hidden.dtype),
            in_specs=[hbm] * 25,
            out_specs=hbm,
            scratch_shapes=[
                pltpu.VMEM((DEPTH, FF, 256), BF16),
                pltpu.VMEM((2, ROWS, KEYS, 2 * HKV), BF16),
                pltpu.VMEM((ROWS, CTOK, DIM), BF16),
                pltpu.VMEM((CTOK, DIM), BF16),
                pltpu.VMEM((CTOK, FFH), BF16),
                pltpu.VMEM((2, CTOK, FFH), BF16),
                pltpu.VMEM((ROWS, 4, CTOK, HEAD_DIM), BF16),
                pltpu.VMEM((CTOK, 2 * HQ), BF16),
                pltpu.VMEM((CTOK, DIM), BF16),
                pltpu.VMEM((2, CTOK, DIM), BF16),
                pltpu.VMEM((2, ROWS, TOK, 128), F32),
                pltpu.VMEM((2, ROWS, TOK, 128), F32),
                pltpu.VMEM((2, ROWS, TOK, 128), jnp.int32),
                pltpu.VMEM((8, ROWS, 128), jnp.int32),
                pltpu.VMEM((1, 128), F32),
                pltpu.VMEM((8, 1, DIM), F32),
                *[pltpu.VMEM((DIM,), F32)] * 8,
                pltpu.VMEM((4, CTOK, KEYS), F32),
                pltpu.VMEM((4, CTOK, 128), F32),
                *[pltpu.VMEM((CTOK, 256), F32)] * 4,
                dma((9,)), dma((DEPTH,)), dma((2, 2)), dma((ROWS,)), dma((ROWS,)), dma((ROWS,)),
                dma((8,)), dma((8,)),
                dma((2, ROWS, CHIPS)), dma((2, ROWS, CHIPS)), dma((ROWS, PIECES)), dma((ROWS, PIECES)),
                dma((2,)), dma((2,)), dma, dma,
                dma((2,)), dma((2,)), dma((2, 2)), dma((2, 2)), dma((ROWS,)),
            ],
            compiler_params=pltpu.CompilerParams(
                collective_id=0, has_side_effects=True, vmem_limit_bytes=67043328),
            cost_estimate=pl.CostEstimate(flops=flops, bytes_accessed=600000000, transcendentals=0),
            name="layers",
        )(hidden, positions, freq, *norms, *local_w[:7], *global_w[:7])

    specs_in = tuple([P("dp", "cp"), P("dp", "cp")] + [P()] * 22)
    return jax.shard_map(device_step, mesh=mesh, in_specs=specs_in, out_specs=P("dp", "cp"), check_vma=False)
```

```python
import functools
import math

import jax
import jax.numpy as jnp
import numpy as np
from jax import lax
from jax.experimental import pallas as pl
from jax.experimental.pallas import tpu as pltpu
from jax.sharding import PartitionSpec as P

HEAD_DIM = 256
WINDOW = 512
EPSILON = 1e-6
THETA = 10000.0
SOFT_CAP = 50.0
EXP2_CAP = SOFT_CAP * math.log2(math.e)

MESH = pl.DeviceIdType.MESH
F32 = jnp.float32
BF16 = jnp.bfloat16

ROWS = 3
TOK = 128
CTOK = 256
DIM = 2560
HQ = 1024
HKV = 512
FF = 10240
FFH = FF // 2
DH = DIM // 2
CHIPS = 4
STEPS = 2 * ROWS
DEPTH = 4
GU = FFH // 512
SCORES = 8
NCHUNK = 128
PIECE = 16
PIECES = 8
PTOK = CTOK // PIECES
KEYS = CHIPS * CTOK


def dot(a, b):
    return jnp.dot(a, b, preferred_element_type=F32)


def rms(u, w):
    mean_sq = jnp.mean(u * u, axis=-1, keepdims=True)
    return (u * lax.rsqrt(mean_sq + EPSILON) * (1.0 + w)).astype(BF16)


def gated(g, u):
    g = g.astype(BF16).astype(F32)
    u = u.astype(BF16).astype(F32)
    return (jax.nn.gelu(g, approximate=True) * u).astype(BF16)


def kernel(x_hbm, pos_in, freq_in, n0, n1, n2, n3, n4, n5, n6, n7,
           wq0, wk0, wv0, wo0, wg0, wu0, wd0, wq1, wk1, wv1, wo1, wg1, wu1, wd1,
           out_hbm,
           ring, kvbuf, xbuf, mbuf, hown, hpeer, qbuf, obuf, abuf, dbuf, cosb, sinb, tposb, posbuf, freq, norms, r0, r1, r2, r3, r4, r5, r6, r7, ebuf, sbuf, gs, us, gb, ub,
           n_sem, ring_sem, half_sem, xl_sem, xs_sem, xr_sem, ps_sem, pr_sem, kvs_sem, kvr_sem, ks_sem, kr_sem,
           os_sem, or_sem, as_sem, ar_sem, hs_sem, hr_sem, dss_sem, dr_sem, out_sem):
    me = lax.axis_index("cp")
    chip = me // 2
    core = me % 2
    peer = me + 1 - 2 * core

    def at(dev):
        return {"cp": dev}

    def start_cols(w, rows, col, slot, row0):
        pltpu.make_async_copy(
            w.at[pl.ds(0, rows), pl.ds(pl.multiple_of(col, 256), 256)],
            ring.at[slot, pl.ds(row0, rows), :], ring_sem.at[slot]).start()

    def by_layer(first, f0, f1):
        @pl.when(first)
        def _():
            f0()

        @pl.when(jnp.logical_not(first))
        def _():
            f1()

    def start_gu(first, i, slot):
        def go(wg, wu):
            col = core * FFH + i * 512
            for t in range(2):
                start_cols(wg, DIM, col + 256 * t, slot, 2 * t * DIM)
                start_cols(wu, DIM, col + 256 * t, slot, (2 * t + 1) * DIM)
        by_layer(first, lambda: go(wg0, wu0), lambda: go(wg1, wu1))

    def start_down(first, n, slot):
        def go(wd):
            start_cols(wd, FF, core * DH + n * 256, slot, 0)
        by_layer(first, lambda: go(wd0), lambda: go(wd1))

    def start_wo(first, slot):
        def go(wo):
            for t in range(5):
                start_cols(wo, 2048, core * DH + t * 256, slot, t * 2048)
        by_layer(first, lambda: go(wo0), lambda: go(wo1))

    def start_kv(wk, wv, slot):
        for t in range(2):
            start_cols(wk, DIM, core * HKV + t * 256, slot, t * DIM)
            start_cols(wv, DIM, core * HKV + t * 256, slot, (2 + t) * DIM)

    def start_q(wq, slot):
        for t in range(4):
            start_cols(wq, DIM, core * HQ + t * 256, slot, t * DIM)

    def wait_w(slot):
        pltpu.make_async_copy(wd0.at[:, pl.ds(0, 256)], ring.at[slot], ring_sem.at[slot]).wait()

    def unit(slot, t, rows=DIM):
        return ring[slot, pl.ds(t * rows, rows), :]

    def x_local(r):
        return pltpu.make_async_copy(
            x_hbm.at[r], xbuf.at[r, pl.ds(pl.multiple_of(core * TOK, TOK), TOK), :], xl_sem.at[r])

    def x_remote(r):
        return pltpu.make_async_remote_copy(
            x_hbm.at[r], xbuf.at[r, pl.ds(pl.multiple_of(core * TOK, TOK), TOK), :],
            xs_sem.at[r], xr_sem.at[r], device_id=at(peer), device_id_type=MESH)

    def norm_copy(k, src):
        return pltpu.make_async_copy(src, nraw[k], n_sem.at[k])

    all_norms = (n0, n1, n2, n3, n4, n5, n6, n7)
    nraw = (r0, r1, r2, r3, r4, r5, r6, r7)

    def freq_copy():
        return pltpu.make_async_copy(freq_in, freq, n_sem.at[8])

    def tables(c):
        rows = posbuf[2 * chip + c].astype(F32)
        cols = jnp.transpose(jnp.concatenate([rows, jnp.zeros((TOK - ROWS, TOK), F32)], axis=0))
        for r in range(ROWS):
            col = jnp.broadcast_to(cols[:, r:r + 1], (TOK, 128))
            tposb[c, r] = col.astype(jnp.int32)
            angle = col * freq[...]
            cosb[c, r] = jnp.cos(angle)
            sinb[c, r] = jnp.sin(angle)

    def pos_local():
        return pltpu.make_async_copy(pos_in, posbuf.at[me], ps_sem.at[0])

    def pos_remote(k):
        return pltpu.make_async_remote_copy(
            pos_in, posbuf.at[me], ps_sem.at[k], pr_sem.at[k],
            device_id=at(lax.rem(me + k, 8)), device_id_type=MESH)

    def kv_own(l, r):
        return kvbuf.at[l, r, pl.ds(pl.multiple_of(chip * CTOK, CTOK), CTOK), :]

    def kv_remote(l, r, d):
        return pltpu.make_async_remote_copy(
            kv_own(l, r), kv_own(l, r), kvs_sem.at[l, r, d], kvr_sem.at[l, r, d],
            device_id=at(lax.rem(me + 2 * d, 8)), device_id_type=MESH)

    def kv_piece(r, h):
        return kvbuf.at[0, r, pl.ds(pl.multiple_of(CTOK + h * PTOK, PTOK), PTOK), :]

    def kv_second(r, h):
        return pltpu.make_async_remote_copy(
            kv_piece(r, h), kv_piece(r, h), ks_sem.at[r, h], kr_sem.at[r, h],
            device_id=at(6 + core), device_id_type=MESH)

    def kv_relay(r, h):
        return pltpu.make_async_remote_copy(
            kv_piece(r, h), kv_piece(r, h), ks_sem.at[r, h], kr_sem.at[r, h],
            device_id=at(4 + core), device_id_type=MESH)

    def forward(r, h):
        @pl.when(chip == 3)
        def _():
            kv_second(r, h).wait_recv()
            kv_relay(r, h).start()

    def send_kv0(r):
        @pl.when(chip == 0)
        def _():
            kv_remote(0, r, 2).start()
            kv_remote(0, r, 1).start()

        @pl.when(chip == 1)
        def _():
            for h in range(PIECES):
                kv_second(r, h).start()

        @pl.when(chip == 2)
        def _():
            kv_remote(0, r, 1).start()

    def half(buf, width):
        return buf.at[:, pl.ds(pl.multiple_of(core * width, 256), width)]

    def o_remote(kh):
        cols = obuf.at[:, pl.ds(pl.multiple_of(core * HQ + kh * 512, 512), 512)]
        return pltpu.make_async_remote_copy(
            cols, cols, os_sem.at[kh], or_sem.at[kh], device_id=at(peer), device_id_type=MESH)

    def a_remote(k):
        width = 768 - 256 * k
        cols = abuf.at[:, pl.ds(pl.multiple_of(core * DH + k * 768, 256), width)]
        return pltpu.make_async_remote_copy(
            cols, cols, as_sem.at[k], ar_sem.at[k], device_id=at(peer), device_id_type=MESH)

    def d_remote(par, k):
        width = 768 - 256 * k
        cols = dbuf.at[par, :, pl.ds(pl.multiple_of(core * DH + k * 768, 256), width)]
        return pltpu.make_async_remote_copy(
            cols, cols, dss_sem.at[par, k], dr_sem.at[par, k], device_id=at(peer), device_id_type=MESH)

    def h_remote(par, i):
        cols = pl.ds(pl.multiple_of(i * 512, 512), 512)
        return pltpu.make_async_remote_copy(
            hown.at[:, cols], hpeer.at[par, :, cols], hs_sem.at[par], hr_sem.at[par],
            device_id=at(peer), device_id_type=MESH)

    def h_all(par):
        return pltpu.make_async_remote_copy(
            hown, hpeer.at[par], hs_sem.at[par], hr_sem.at[par], device_id=at(peer), device_id_type=MESH)

    def rope(y, r, t, dst):
        y = y.astype(BF16).astype(F32)
        for c in range(2):
            f = y[c * TOK:(c + 1) * TOK, :128]
            s = y[c * TOK:(c + 1) * TOK, 128:]
            cos = cosb[c, r]
            sin = sinb[c, r]
            dst(c, (f * cos - s * sin) * t, (s * cos + f * sin) * t)

    def kv_part(src, slot, l, r):
        for t in range(2):
            y = dot(src(), unit(slot, t))

            def put(c, a, b, t=t):
                rows = pl.ds(pl.multiple_of(chip * CTOK + c * TOK, TOK), TOK)
                kvbuf[l, r, rows, t * 256:t * 256 + 128] = a.astype(BF16)
                kvbuf[l, r, rows, t * 256 + 128:t * 256 + 256] = b.astype(BF16)
            rope(y, r, 1.0, put)
            kvbuf[l, r, pl.ds(pl.multiple_of(chip * CTOK, CTOK), CTOK), HKV + t * 256:HKV + t * 256 + 256] = dot(src(), unit(slot, 2 + t)).astype(BF16)

    def q_part(src, slot, r):
        for t in range(4):
            y = dot(src(), unit(slot, t))

            def put(c, a, b, t=t):
                rows = pl.ds(c * TOK, TOK)
                qbuf[r, t, rows, 0:128] = a.astype(BF16)
                qbuf[r, t, rows, 128:256] = b.astype(BF16)
            rope(y, r, HEAD_DIM ** -0.5, put)

    def send_kv(l, r, far):
        for d in range(1, far + 1):
            @pl.when(chip + d < CHIPS)
            def _(d=d):
                kv_remote(l, r, d).start()

    def kv_wait(j):
        l = j // ROWS
        r = j % ROWS
        for d in range(1, CHIPS):
            @pl.when((chip - d >= 0) & (l == 1))
            def _(d=d):
                kv_remote(1, r, d).wait_recv()

        @pl.when(l == 0)
        def _():
            @pl.when((chip == 1) | (chip == 3))
            def _():
                kv_remote(0, r, 1).wait_recv()

            @pl.when(chip == 2)
            def _():
                kv_remote(0, r, 2).wait_recv()
                for h in range(PIECES):
                    kv_relay(r, h).wait_recv()

    def score(j, kh, t, fresh):
        l = j // ROWS
        r = j % ROWS
        reach = WINDOW + l * 1000000
        k = kvbuf[l, r, pl.ds(pl.multiple_of(t * CTOK, CTOK), CTOK), pl.ds(pl.multiple_of(kh * 256, 256), 256)]
        masks = {}
        for c in range(2):
            for kc in range(2):
                off = tposb[c, r] - posbuf[2 * t + kc, pl.ds(r, 1), :]
                masks[c, kc] = (off >= 0) & (off < reach)
        for hh in range(2):
            q = qbuf[r, 2 * kh + hh]
            s = lax.dot_general(q, k, (((1,), (1,)), ((), ())), preferred_element_type=F32)
            e = jnp.exp2(EXP2_CAP * jnp.tanh(s * (1.0 / SOFT_CAP)))
            for c in range(2):
                rows = slice(c * TOK, (c + 1) * TOK)
                tot = jnp.where(fresh, 0.0, sbuf[2 * kh + hh, rows, :])
                for kc in range(2):
                    piece = jnp.where(masks[c, kc], e[rows, kc * 128:(kc + 1) * 128], 0.0)
                    ebuf[2 * kh + hh, rows, pl.ds(pl.multiple_of(t * CTOK + kc * 128, 128), 128)] = piece
                    tot = tot + piece
                sbuf[2 * kh + hh, rows, :] = tot

    def mix(j, kh):
        l = j // ROWS
        r = j % ROWS
        v = kvbuf[l, r, :, pl.ds(pl.multiple_of(HKV + kh * 256, 256), 256)]
        for hh in range(2):
            inv = 1.0 / jnp.sum(sbuf[2 * kh + hh], axis=-1, keepdims=True)
            p = (ebuf[2 * kh + hh] * inv).astype(BF16)
            col = pl.multiple_of(core * HQ + (2 * kh + hh) * 256, 256)
            obuf[:, pl.ds(col, 256)] = dot(p, v).astype(BF16)

    def attention():
        zero = 0 * me

        def block(t, fresh):
            def go(kh, carry):
                score(zero, kh, t, fresh)
                return carry
            with jax.named_scope("att"):
                lax.fori_loop(0, 2, go, 0)

        def hop(d):
            return lax.rem(chip + CHIPS - d, CHIPS)
        block(chip, me >= 0)
        block(hop(3), me < 0)
        with jax.named_scope("att_wait"):
            @pl.when(chip == 2)
            def _():
                kv_remote(0, zero, 2).wait_recv()
            forward(0, 7)
        block(hop(2), me < 0)
        with jax.named_scope("att_wait"):
            @pl.when((chip == 1) | (chip == 3))
            def _():
                kv_remote(0, zero, 1).wait_recv()

            @pl.when(chip == 2)
            def _():
                for h in range(PIECES):
                    kv_relay(zero, h).wait_recv()
        block(hop(1), me < 0)
        with jax.named_scope("att"):
            def go2(kh, carry):
                mix(zero, kh)
                o_remote(kh).start()
                return carry
            lax.fori_loop(0, 2, go2, 0)

    def out_proj(slot):
        with jax.named_scope("o_wait"):
            for kh in range(2):
                o_remote(kh).wait()
        with jax.named_scope("wo_wait"):
            wait_w(slot)
        for t in range(5):
            col = pl.multiple_of(core * DH + t * 256, 256)
            abuf[:, pl.ds(col, 256)] = dot(obuf[...], unit(slot, t, 2048)).astype(BF16)
            if t == 2:
                a_remote(0).start()
        a_remote(1).start()

    def mid_rows(j, base, keep=None):
        l = j // ROWS
        r = j % ROWS
        for t in range(0, NCHUNK, PIECE):
            rows = pl.ds(pl.multiple_of(base + t, PIECE), PIECE)
            y = rms(abuf[rows, :].astype(F32), norms[4 * l + 1])
            x = xbuf[r, rows, :]
            x1 = (x.astype(F32) + y.astype(F32)).astype(BF16)
            xbuf[r, rows, :] = x1 if keep is None else jnp.where(keep, x1, x)
            mbuf[rows, :] = rms(x1.astype(F32), norms[4 * l + 2])

    def end_rows(j, par, base, keep=None):
        l = j // ROWS
        r = j % ROWS
        for t in range(0, NCHUNK, PIECE):
            rows = pl.ds(pl.multiple_of(base + t, PIECE), PIECE)
            y = rms(dbuf[par, rows, :].astype(F32), norms[4 * l + 3])
            x = xbuf[r, rows, :]
            x2 = (x.astype(F32) + y.astype(F32)).astype(BF16)
            xbuf[r, rows, :] = x2 if keep is None else jnp.where(keep, x2, x)
            dbuf[par, rows, :] = rms(x2.astype(F32), norms[4])

    def put_out(j):
        r = j % ROWS
        return pltpu.make_async_copy(
            xbuf.at[r, pl.ds(pl.multiple_of(core * TOK, TOK), TOK), :], out_hbm.at[r], out_sem.at[r])

    pos_local().start()
    x_local(0).start()
    freq_copy().start()
    for k in range(8):
        norm_copy(k, all_norms[k]).start()
    x_local(1).start()
    x_local(2).start()
    def clear(i, carry):
        l = i // (ROWS * CHIPS)
        r = (i // CHIPS) % ROWS
        b = i % CHIPS

        @pl.when((b > chip) | ((l == 0) & (b < chip - 2)))
        def _():
            kvbuf[l, r, pl.ds(pl.multiple_of(b * CTOK, CTOK), CTOK), HKV:] = jnp.zeros((CTOK, HKV), BF16)
        return carry
    lax.fori_loop(0, 2 * ROWS * CHIPS, clear, 0)
    freq_copy().wait()
    pos_local().wait()
    start_kv(wk0, wv0, 0)
    with jax.named_scope("tables"):
        tables(core)
    barrier = pltpu.get_barrier_semaphore()
    for k in range(1, 8):
        pl.semaphore_signal(barrier, inc=1, device_id=at(lax.rem(me + k, 8)), device_id_type=MESH)
    with jax.named_scope("entry"):
        pl.semaphore_wait(barrier, 7)
    x_remote(0).start()
    for k in range(1, 8):
        pos_remote(k).start()
    for r in range(1, ROWS):
        x_remote(r).start()
    for k in range(8):
        norm_copy(k, all_norms[k]).wait()
    for k in range(8):
        norms[k] = nraw[k][...].reshape(1, DIM)

    @pl.when(core == 0)
    def _():
        pos_remote(7).wait_recv()

    @pl.when(core == 1)
    def _():
        pos_remote(1).wait_recv()
    with jax.named_scope("tables"):
        tables(1 - core)
    start_q(wq0, 1)
    start_wo(me >= 0, 2)

    def first_norm(r, carry):
        with jax.named_scope("x_wait"):
            x_local(r).wait()
            x_remote(r).wait()

        def chunk(i, carry):
            for t in range(0, NCHUNK, PIECE):
                rows = pl.ds(pl.multiple_of(i * NCHUNK + t, PIECE), PIECE)
                hpeer[r // 2, rows, pl.ds(pl.multiple_of((r % 2) * DIM, DIM), DIM)] = rms(
                    xbuf[r, rows, :].astype(F32), norms[0])
            return carry
        lax.fori_loop(0, CTOK // NCHUNK, chunk, 0)
        return carry

    start_gu(me >= 0, 0, 3)
    wait_w(0)

    def a0(r):
        return hpeer[r // 2, :, pl.ds(pl.multiple_of((r % 2) * DIM, DIM), DIM)]

    def first_kv(r, carry):
        first_norm(r, 0)
        kv_part(lambda: a0(r), 0, 0, r)
        send_kv0(r)
        return carry
    with jax.named_scope("first_kv"):
        lax.fori_loop(0, ROWS, first_kv, 0)
    start_gu(me >= 0, 1, 0)
    wait_w(1)

    def first_q(r, carry):
        q_part(lambda: a0(r), 1, r)

        forward(0, 2 * r + 2)

        @pl.when(r <= 1)
        def _():
            forward(0, 2 * r + 3)
        return carry
    forward(0, 0)
    forward(0, 1)
    with jax.named_scope("first_q"):
        lax.fori_loop(0, ROWS, first_q, 0)
    start_gu(me >= 0, 2, 1)
    for k in range(1, 8):
        pos_remote(k).wait_send()

    @pl.when(core == 0)
    def _():
        for k in range(1, 7):
            pos_remote(k).wait_recv()

    @pl.when(core == 1)
    def _():
        for k in range(2, 8):
            pos_remote(k).wait_recv()
    attention()
    for h in range(4):
        forward(1, h)
    out_proj(2)
    forward(1, 4)
    forward(1, 5)
    with jax.named_scope("a_wait"):
        for k in range(2):
            a_remote(k).wait()

    def first_mid(i, carry):
        mid_rows(0 * me, i * NCHUNK)
        return carry
    lax.fori_loop(0, CTOK // NCHUNK, first_mid, 0)
    forward(1, 6)
    forward(1, 7)

    def step(j, carry):
        first = j < ROWS
        first_next = j + 1 < ROWS
        more = j + 1 < STEPS
        par = j % 2
        has_qkv = (j >= 1) & (j <= ROWS)
        done = jnp.where(j >= 1, jnp.minimum(j - 1, ROWS), 0)
        extra = jnp.where(has_qkv, 2, 0)
        sb = 3 + 2 * done
        db = sb + extra + GU
        nxt = jnp.minimum(j + 1, STEPS - 1)

        def sl(p):
            return lax.rem(p, DEPTH)

        def gate_up(i, pos, beside):
            slot = sl(pos)
            with jax.named_scope("gu_wait"):
                wait_w(slot)
            base = i * 512
            prev = base - 256 if not isinstance(i, int) or i > 0 else base + 256
            hown[:, pl.ds(pl.multiple_of(prev, 256), 256)] = gated(gs[...], us[...])
            g = dot(mbuf[...], unit(slot, 0))
            u = dot(mbuf[...], unit(slot, 1))
            beside()
            hown[:, pl.ds(pl.multiple_of(base, 256), 256)] = gated(g, u)
            gs[...] = dot(mbuf[...], unit(slot, 2))
            us[...] = dot(mbuf[...], unit(slot, 3))

        @pl.when(has_qkv)
        def _():
            start_q(wq1, sl(sb + 3))

        @pl.when(jnp.logical_not(has_qkv))
        def _():
            start_gu(first, 3, sl(sb + 3))
        with jax.named_scope("gate_up0"):
            gate_up(0, sb, lambda: None)

        @pl.when(has_qkv)
        def _():
            start_gu(first, 2, sl(sb + 4))

        @pl.when(jnp.logical_not(has_qkv))
        def _():
            start_gu(first, 4, sl(sb + 4))

        @pl.when(j >= 1)
        def _():
            with jax.named_scope("d_wait"):
                for k in range(2):
                    d_remote(1 - par, k).wait()
        last = jnp.maximum(j - 1, 0)

        def ending():
            for c in range(2):
                end_rows(last, 1 - par, c * NCHUNK, j >= 1)
        with jax.named_scope("gate_up1"):
            gate_up(1, sb + 1, ending)

        @pl.when(has_qkv)
        def _():
            start_gu(first, 3, sl(sb + 5))
            wait_w(sl(sb + 2))
            with jax.named_scope("kv"):
                kv_part(lambda: dbuf[1 - par], sl(sb + 2), 1, last)
            send_kv(1, last, 3)
            start_gu(first, 4, sl(sb + 6))
            wait_w(sl(sb + 3))
            with jax.named_scope("q"):
                q_part(lambda: dbuf[1 - par], sl(sb + 3), last)

        @pl.when(j > ROWS)
        def _():
            put_out(j - 1).start()

        @pl.when(more)
        def _():
            with jax.named_scope("att_wait"):
                kv_wait(j + 1)

        def scoring(i, carry):
            pos = sb + extra + i

            @pl.when(i + 3 < GU)
            def _():
                start_gu(first, i + 3, sl(pos + 3))

            @pl.when(i + 3 >= GU)
            def _():
                start_down(first, i + 3 - GU, sl(pos + 3))
            h_remote(par, i - 2).start()
            e = i - 2
            gate_up(i, pos, lambda: score(nxt, e // CHIPS, e % CHIPS, e % CHIPS == 0))
            return carry
        with jax.named_scope("gate_up"):
            lax.fori_loop(2, GU, scoring, 0)

        hown[:, FFH - 256:FFH] = gated(gs[...], us[...])
        h_remote(par, GU - 2).start()
        h_remote(par, GU - 1).start()

        @pl.when(j == 0)
        def _():
            for h in range(PIECES):
                forward(2, h)

        def down_col(n):
            return pl.ds(pl.multiple_of(core * DH + n * 256, 256), 256)

        mine = pl.ds(pl.multiple_of(core * FFH, FFH), FFH)
        other = pl.ds(pl.multiple_of((1 - core) * FFH, FFH), FFH)
        def pair(lhs, sa, sb_, rows, out_a, out_b):
            y = dot(lhs, jnp.concatenate([ring[sa, rows, :], ring[sb_, rows, :]], axis=1))
            out_a[...] = y[:, :256]
            out_b[...] = y[:, 256:]

        def half_down(n, pos, k):
            row = pl.multiple_of((core + k - 2 * core * k) * FFH, FFH)

            def go(wd):
                pltpu.make_async_copy(
                    wd.at[pl.ds(row, FFH), pl.ds(pl.multiple_of(core * DH + n * 256, 256), 256)],
                    ring.at[sl(pos), pl.ds(row, FFH), :], half_sem.at[k, n - 3]).start()
            by_layer(first, lambda: go(wd0), lambda: go(wd1))

        def half_wait(n, pos, k):
            row = pl.multiple_of((core + k - 2 * core * k) * FFH, FFH)
            pltpu.make_async_copy(
                wd0.at[pl.ds(row, FFH), pl.ds(0, 256)], ring.at[sl(pos), pl.ds(row, FFH), :],
                half_sem.at[k, n - 3]).wait()

        p3 = db + 3 + jnp.where(more, 1, 0)
        p4 = p3 + 1
        with jax.named_scope("down_a"):
            @pl.when(more)
            def _():
                start_wo(first_next, sl(db + 3))

            @pl.when(jnp.logical_not(more))
            def _():
                half_down(3, p3, 0)
                half_down(3, p3, 1)
            wait_w(sl(db))
            wait_w(sl(db + 1))
            pair(hown[...], sl(db), sl(db + 1), mine, gs, us)
            mix(nxt, 0)

            @pl.when(more)
            def _():
                o_remote(0).start()
                half_down(3, p3, 0)
            half_down(4, p4, 0)
            with jax.named_scope("h_wait"):
                h_all(par).wait()
            pair(hpeer[par], sl(db), sl(db + 1), other, gb, ub)
            mix(nxt, 1)
            dbuf[par, :, down_col(0)] = (gs[...] + gb[...]).astype(BF16)
            dbuf[par, :, down_col(1)] = (us[...] + ub[...]).astype(BF16)

            @pl.when(more)
            def _():
                o_remote(1).start()
                half_down(3, p3, 1)
            half_down(4, p4, 1)

        with jax.named_scope("down2"):
            wait_w(sl(db + 2))
            gs[...] = dot(hown[...], ring[sl(db + 2), mine, :])
            us[...] = dot(hpeer[par], ring[sl(db + 2), other, :])
            dbuf[par, :, down_col(2)] = (gs[...] + us[...]).astype(BF16)
            d_remote(par, 0).start()

        @pl.when(more)
        def _():
            start_gu(first_next, 0, sl(db + 6))
            with jax.named_scope("proj"):
                out_proj(sl(db + 3))
            start_gu(first_next, 1, sl(db + 7))
        s3 = sl(p3)
        s4 = sl(p4)
        with jax.named_scope("down3"):
            with jax.named_scope("dn_wait"):
                half_wait(3, p3, 0)
                half_wait(4, p4, 0)
            pair(hown[...], s3, s4, mine, gs, us)

        @pl.when(more)
        def _():
            with jax.named_scope("a_wait"):
                for k in range(2):
                    a_remote(k).wait()

        with jax.named_scope("down4"):
            with jax.named_scope("dn_wait"):
                half_wait(3, p3, 1)
                half_wait(4, p4, 1)
            pair(hpeer[par], s3, s4, other, gb, ub)
            for c in range(2):
                mid_rows(nxt, c * NCHUNK, more)
            dbuf[par, :, down_col(3)] = (gs[...] + gb[...]).astype(BF16)
            dbuf[par, :, down_col(4)] = (us[...] + ub[...]).astype(BF16)

        @pl.when(more)
        def _():
            @pl.when(j + 1 <= ROWS)
            def _():
                start_kv(wk1, wv1, sl(db + 8))

            @pl.when(j + 1 > ROWS)
            def _():
                start_gu(first_next, 2, sl(db + 8))
        d_remote(par, 1).start()
        return carry

    lax.fori_loop(0, STEPS, step, 0)

    for k in range(2):
        d_remote((STEPS - 1) % 2, k).wait()

    def final(i, carry):
        end_rows(STEPS - 1 + 0 * me, (STEPS - 1) % 2, core * TOK + i * NCHUNK)
        return carry
    lax.fori_loop(0, TOK // NCHUNK, final, 0)
    put_out(STEPS - 1).start()
    for r in range(ROWS):
        put_out(r).wait()
    for r in range(ROWS):
        for d in range(1, CHIPS):
            @pl.when(chip + d < CHIPS)
            def _(r=r, d=d):
                kv_remote(1, r, d).wait_send()

        @pl.when(chip == 0)
        def _(r=r):
            kv_remote(0, r, 2).wait_send()

        @pl.when((chip == 0) | (chip == 2))
        def _(r=r):
            kv_remote(0, r, 1).wait_send()

        @pl.when(chip == 1)
        def _(r=r):
            for h in range(PIECES):
                kv_second(r, h).wait_send()

        @pl.when(chip == 3)
        def _(r=r):
            for h in range(PIECES):
                kv_relay(r, h).wait_send()


def solution(mesh):
    def device_step(hidden, positions, *weights):
        local_w = weights[:11]
        global_w = weights[11:]
        half_dim = HEAD_DIM // 2
        inv_freq = (THETA ** (-(np.arange(half_dim, dtype=np.float64) * 2.0 / HEAD_DIM))).astype(np.float32)
        freq = jnp.asarray(inv_freq.reshape(1, half_dim))
        norms = local_w[7:11] + global_w[7:11]
        hbm = pl.BlockSpec(memory_space=pltpu.HBM)
        dma = pltpu.SemaphoreType.DMA
        flops = 2 * ROWS * TOK * 2 * (DIM * 4096 + 2048 * DIM + 3 * DIM * FF)
        return pl.pallas_call(
            kernel,
            out_shape=jax.ShapeDtypeStruct(hidden.shape, hidden.dtype),
            in_specs=[hbm] * 25,
            out_specs=hbm,
            scratch_shapes=[
                pltpu.VMEM((DEPTH, FF, 256), BF16),
                pltpu.VMEM((2, ROWS, KEYS, 2 * HKV), BF16),
                pltpu.VMEM((ROWS, CTOK, DIM), BF16),
                pltpu.VMEM((CTOK, DIM), BF16),
                pltpu.VMEM((CTOK, FFH), BF16),
                pltpu.VMEM((2, CTOK, FFH), BF16),
                pltpu.VMEM((ROWS, 4, CTOK, HEAD_DIM), BF16),
                pltpu.VMEM((CTOK, 2 * HQ), BF16),
                pltpu.VMEM((CTOK, DIM), BF16),
                pltpu.VMEM((2, CTOK, DIM), BF16),
                pltpu.VMEM((2, ROWS, TOK, 128), F32),
                pltpu.VMEM((2, ROWS, TOK, 128), F32),
                pltpu.VMEM((2, ROWS, TOK, 128), jnp.int32),
                pltpu.VMEM((8, ROWS, 128), jnp.int32),
                pltpu.VMEM((1, 128), F32),
                pltpu.VMEM((8, 1, DIM), F32),
                *[pltpu.VMEM((DIM,), F32)] * 8,
                pltpu.VMEM((4, CTOK, KEYS), F32),
                pltpu.VMEM((4, CTOK, 128), F32),
                *[pltpu.VMEM((CTOK, 256), F32)] * 4,
                dma((9,)), dma((DEPTH,)), dma((2, 2)), dma((ROWS,)), dma((ROWS,)), dma((ROWS,)),
                dma((8,)), dma((8,)),
                dma((2, ROWS, CHIPS)), dma((2, ROWS, CHIPS)), dma((ROWS, PIECES)), dma((ROWS, PIECES)),
                dma((2,)), dma((2,)), dma((2,)), dma((2,)),
                dma((2,)), dma((2,)), dma((2, 2)), dma((2, 2)), dma((ROWS,)),
            ],
            compiler_params=pltpu.CompilerParams(
                collective_id=0, has_side_effects=True, vmem_limit_bytes=67043328),
            cost_estimate=pl.CostEstimate(flops=flops, bytes_accessed=600000000, transcendentals=0),
            name="layers",
        )(hidden, positions, freq, *norms, *local_w[:7], *global_w[:7])

    specs_in = tuple([P("dp", "cp"), P("dp", "cp")] + [P()] * 22)
    return jax.shard_map(device_step, mesh=mesh, in_specs=specs_in, out_specs=P("dp", "cp"), check_vma=False)
```
